32 devices in a mesh: grp: 16 (over z, y, x), rep: 2 (over core).
Axes of the slice: x: 2, y: 2, z: 4, core: 2. Of those that a mesh axis runs over, the one named last changes fastest.
Arguments:
- snapshots: float32 [16, 2048, 1024], P('grp', 'rep'), may hold values from -6 to 6
- row_factor: float32 [2048, 128], P('rep'), may hold values from -0.125 to 0.125
- time_factor: float32 [16, 8], replicated, may hold values from -1.5 to 1.5
Outputs:
- new_rows: float32 [2048, 128], P('rep')
- new_time: float32 [16, 8], replicated
The draws below stay inside these ranges and needn't reach their ends.
All inputs are finite; a program needn't handle non-finite values.
Results may differ from the reference program's by a relative error of at most 0.0001.
Values sent between devices are 32-bit elements; how exact they have to be, the bound alone decides.
No kernel may reach another device: no remote copies, remote signals or barrier semaphores. Data moves between devices by JAX's collectives and lax.ppermute only.
A program may use at most 64 MiB of HBM per device.

```python
import math
import jax
import jax.numpy as jnp
from jax import lax

ROWS = 2048
COLS = 1024
RANK_ROW = 128
STEPS = 8
SNAPS = 16
RANK_TIME = 8


def steps_of(key, dims, cuts, low, high):
    gain, own = 1.0, jax.random.fold_in(key, 6)
    for dim, shards_of in cuts:
        draws = jnp.exp(jax.random.uniform(jax.random.fold_in(own, dim), (shards_of,), jnp.float32, low / len(cuts), high / len(cuts)))
        gain = gain * jnp.repeat(draws, dims[dim] // shards_of).reshape([-1 if axis == dim else 1 for axis in range(len(dims))])
    return gain


def normal_values(own_key, shape, deviation, limit, shards=(), held_as=jnp.bfloat16):
    factor_of = steps_of(own_key, shape, shards, -0.22, 0.18) if shards else 1.0
    entries = jax.random.normal(own_key, shape, jnp.float32) * deviation * factor_of
    return jnp.minimum(jnp.maximum(entries, -limit), limit).astype(held_as)


def setup_inputs(seed: int = 0) -> dict:
    splits = jax.random.split(jax.random.key(seed), 4)
    return {
        "snapshots": normal_values(splits[0], (SNAPS, ROWS, COLS), 1.0, 6.0, ((0, 16), (1, 2)), jnp.float32),
        "row_factor": normal_values(splits[1], (ROWS, RANK_ROW), ROWS ** -0.5, 0.125, ((0, 2),), jnp.float32),
        "time_factor": normal_values(splits[2], (SNAPS, RANK_TIME), SNAPS ** -0.5, 1.5, (), jnp.float32),
    }


def highdot(left, right):
    return jnp.dot(left, right, precision=lax.Precision.HIGHEST, preferred_element_type=jnp.float32)

def orthogonalize(start_matrix):
    total = jnp.sum(start_matrix * start_matrix)
    iterate = start_matrix / jnp.sqrt(total + 1e-06)
    for step_index in range(STEPS):
        inner = highdot(iterate.T, iterate)
        iterate = 1.5 * iterate - 0.5 * highdot(iterate, inner)
    return iterate

def reference(snapshots, row_factor, time_factor):
    projected = jnp.einsum('tij,ia->tja', snapshots, row_factor, precision=lax.Precision.HIGHEST)
    flat = projected.reshape(SNAPS, COLS * RANK_ROW)
    gram_total = jnp.dot(flat, flat.T, precision=lax.Precision.HIGHEST, preferred_element_type=jnp.float32)
    start_time = highdot(gram_total, time_factor)
    basis_time = orthogonalize(start_time)
    mixer = highdot(basis_time, basis_time.T)
    weights = highdot(mixer, flat).reshape(SNAPS, COLS, RANK_ROW)
    product = jnp.einsum('tij,tja->ia', snapshots, weights, precision=lax.Precision.HIGHEST)
    new_rows = orthogonalize(product) * math.sqrt(ROWS)
    new_time = basis_time * math.sqrt(SNAPS)
    return (new_rows, new_time)
```

```python
import math

import jax
import jax.numpy as jnp
from jax import lax
from jax.sharding import PartitionSpec as P

STEPS = 8
HIGHEST = lax.Precision.HIGHEST
HIGH = lax.Precision.HIGH


def highdot(left, right):
    return jnp.dot(left, right, precision=HIGHEST, preferred_element_type=jnp.float32)


def orthogonalize(start_matrix):
    total = jnp.sum(start_matrix * start_matrix)
    iterate = start_matrix / jnp.sqrt(total + 1e-06)
    for step_index in range(STEPS):
        inner = highdot(iterate.T, iterate)
        iterate = 1.5 * iterate - 0.5 * highdot(iterate, inner)
    return iterate


def orth_factor(gram):
    rank = gram.shape[0]
    eye = jnp.eye(rank, dtype=jnp.float32)
    total = jnp.sum(gram * eye) + 1e-06
    squared = gram / total
    factor = eye / jnp.sqrt(total)
    for step_index in range(STEPS):
        turn = 1.5 * eye - 0.5 * squared
        factor = highdot(factor, turn)
        if step_index < STEPS - 1:
            squared = highdot(highdot(squared, turn), turn)
    return factor


def sum_of_small(part, axes, devices):
    if devices * part.size > 1 << 20:
        return lax.psum(part, axes)
    copies = jnp.broadcast_to(part.reshape(1, -1), (devices, part.size))
    received = lax.all_to_all(copies, axes, split_axis=0, concat_axis=0, tiled=True)
    return jnp.sum(received, axis=0).reshape(part.shape)


def make_on_device(groups_n, reps):
    half_n = groups_n // 2
    halves = [[h * half_n + i for i in range(half_n)] for h in range(2)]
    across = [(i, (i + half_n) % groups_n) for i in range(groups_n)]
    swap = [(0, 1), (1, 0)]

    def on_device(snapshots, row_factor, time_factor):
        rows, cols = snapshots.shape[1:]
        rank = row_factor.shape[1]
        width = cols // reps
        me = lax.axis_index("rep")
        image = snapshots[0]
        projected = jnp.einsum("ij,ia->aj", image, row_factor, precision=HIGH, preferred_element_type=jnp.float32)
        keep = lax.dynamic_slice_in_dim(projected, me * width, width, 1)
        send = lax.dynamic_slice_in_dim(projected, (1 - me) * width, width, 1)
        summed = keep + lax.ppermute(send, "rep", swap)
        owned = lax.all_to_all(
            summed.reshape(groups_n, rank // groups_n, width), "grp", split_axis=0, concat_axis=0, tiled=True
        )
        flat = owned.reshape(groups_n, -1)
        gram_total = sum_of_small(highdot(flat, flat.T), ("grp", "rep"), groups_n * reps)
        basis_time = orthogonalize(highdot(gram_total, time_factor))
        mixer = highdot(basis_time, basis_time.T)
        weights = highdot(mixer, flat).reshape(owned.shape)
        mine = lax.all_to_all(weights, "grp", split_axis=0, concat_axis=0, tiled=True).reshape(rank, width)
        other = lax.ppermute(mine, "rep", swap)
        left = jnp.where(me == 0, mine, other)
        right = jnp.where(me == 0, other, mine)
        full = jnp.concatenate([left, right], axis=1)
        product = jnp.einsum("ij,aj->ia", image, full, precision=HIGH, preferred_element_type=jnp.float32)
        parts = lax.all_to_all(
            product.reshape(half_n, rows // half_n, rank),
            "grp",
            split_axis=0,
            concat_axis=0,
            tiled=True,
            axis_index_groups=halves,
        )
        chunk = jnp.sum(parts, axis=0)
        chunk = chunk + lax.ppermute(chunk, "grp", across)
        block = lax.all_to_all(
            jnp.broadcast_to(chunk[None], (half_n,) + chunk.shape),
            "grp",
            split_axis=0,
            concat_axis=0,
            tiled=True,
            axis_index_groups=halves,
        ).reshape(rows, rank)
        gram = highdot(block.T, block)
        gram = gram + lax.ppermute(gram, "rep", swap)
        new_rows = highdot(block, orth_factor(gram) * math.sqrt(rows * reps))
        return (new_rows, basis_time * math.sqrt(groups_n))

    return on_device


def solution(mesh):
    return jax.shard_map(
        make_on_device(mesh.shape["grp"], mesh.shape["rep"]),
        mesh=mesh,
        in_specs=(P("grp", "rep", None), P("rep", None), P()),
        out_specs=(P("rep", None), P()),
        check_vma=False,
    )
```

```python
import functools
import math

import jax
import jax.numpy as jnp
from jax import lax
from jax.experimental import pallas as pl
from jax.experimental.pallas import tpu as pltpu
from jax.sharding import PartitionSpec as P

STEPS = 8
F32 = jnp.float32
BF16 = jnp.bfloat16
TINY = 1e-06


def dot(left, right, contract=((1,), (0,))):
    return lax.dot_general(
        left, right, (contract, ((), ())), precision=lax.Precision.HIGHEST, preferred_element_type=F32
    )


def fastdot(left, right, contract):
    return lax.dot_general(left, right, (contract, ((), ())), preferred_element_type=F32)


def split(value):
    high = value.astype(BF16)
    return high, (value - high.astype(F32)).astype(BF16)


def eye(size):
    return (lax.broadcasted_iota(jnp.int32, (size, size), 0) == lax.broadcasted_iota(jnp.int32, (size, size), 1)).astype(F32)


def orth_factor(gram):
    unit = eye(gram.shape[0])
    total = jnp.sum(gram * unit) + TINY
    squared = gram * (1.0 / total)
    factor = unit * lax.rsqrt(total)
    for step_index in range(STEPS):
        turn = 1.5 * unit - 0.5 * squared
        factor = dot(factor, turn)
        if step_index < STEPS - 1:
            squared = dot(dot(squared, turn), turn)
    return factor


def project_kernel(which_ref, image_ref, factor_ref, out_ref):
    image_high, image_low = split(image_ref[...])
    factor_high, factor_low = split(factor_ref[...])
    rank = factor_high.shape[1]
    both = jnp.concatenate([factor_high, factor_low], axis=1)
    wide = fastdot(both, image_high, ((0,), (0,)))
    value = wide[:rank] + wide[rank:] + fastdot(factor_high, image_low, ((0,), (0,)))

    @pl.when(pl.program_id(0) == 0)
    def _():
        out_ref[...] = value

    @pl.when(pl.program_id(0) > 0)
    def _():
        out_ref[...] += value


def project(image, row_factor, which, width, blocks=4):
    rows = image.shape[0]
    rank = row_factor.shape[1]
    block = rows // blocks
    return pl.pallas_call(
        project_kernel,
        grid_spec=pltpu.PrefetchScalarGridSpec(
            num_scalar_prefetch=1,
            grid=(blocks,),
            in_specs=[
                pl.BlockSpec((block, width), lambda i, which_ref: (i, which_ref[0])),
                pl.BlockSpec((block, rank), lambda i, which_ref: (i, 0)),
            ],
            out_specs=pl.BlockSpec((rank, width), lambda i, which_ref: (0, 0)),
        ),
        out_shape=jax.ShapeDtypeStruct((rank, width), F32),
        cost_estimate=pl.CostEstimate(
            flops=6 * rows * width * rank, bytes_accessed=4 * rows * (width + rank), transcendentals=0
        ),
        name="project",
    )(which, image, row_factor)


def product_kernel(which_ref, image_ref, weight_ref, *refs):
    out_ref = refs[-1]
    image_high, image_low = split(image_ref[...])
    weight_high, weight_low = split(weight_ref[...])
    rank = weight_high.shape[0]
    both = jnp.concatenate([weight_high, weight_low], axis=0)
    wide = fastdot(image_high, both, ((1,), (1,)))
    value = wide[:, :rank] + wide[:, rank:] + fastdot(image_low, weight_high, ((1,), (1,)))
    if len(refs) > 1:
        value = value + refs[0][...]
    out_ref[...] = value


def multiply(image, weight, which, start=None, blocks=4):
    rows = image.shape[0]
    rank, width = weight.shape
    block = rows // blocks
    out_spec = pl.BlockSpec((block, rank), lambda i, which_ref: (i, 0))
    more = [] if start is None else [start]
    return pl.pallas_call(
        product_kernel,
        grid_spec=pltpu.PrefetchScalarGridSpec(
            num_scalar_prefetch=1,
            grid=(blocks,),
            in_specs=[
                pl.BlockSpec((block, width), lambda i, which_ref: (i, which_ref[0])),
                pl.BlockSpec((rank, width), lambda i, which_ref: (0, 0)),
            ]
            + [out_spec for _ in more],
            out_specs=out_spec,
        ),
        out_shape=jax.ShapeDtypeStruct((rows, rank), F32),
        cost_estimate=pl.CostEstimate(
            flops=6 * rows * width * rank, bytes_accessed=4 * rows * (width + rank), transcendentals=0
        ),
        name="multiply",
    )(which, image, weight, *more)


def spread(groups_n, rank):
    rows = lax.broadcasted_iota(jnp.int32, (rank, groups_n), 0) // (rank // groups_n)
    return (rows == lax.broadcasted_iota(jnp.int32, (rank, groups_n), 1)).astype(F32)


def same_slot(groups_n, rank):
    per = rank // groups_n
    left = lax.broadcasted_iota(jnp.int32, (rank, rank), 0) % per
    right = lax.broadcasted_iota(jnp.int32, (rank, rank), 1) % per
    return left == right


def gram_kernel(owned_ref, out_ref):
    owned = owned_ref[...]
    groups_n = out_ref.shape[0]
    rank = owned.shape[0]
    full = jnp.where(same_slot(groups_n, rank), dot(owned, owned, ((1,), (1,))), 0.0)
    fold = spread(groups_n, rank)
    out_ref[...] = dot(dot(fold, full, ((0,), (0,))), fold)


def small_gram(owned, groups_n):
    return pl.pallas_call(
        gram_kernel, out_shape=jax.ShapeDtypeStruct((groups_n, groups_n), F32), name="small_gram"
    )(owned)


def mix_kernel(gram_ref, time_ref, owned_ref, out_ref, time_out_ref):
    groups_n = gram_ref.shape[0]
    rank = owned_ref.shape[0]
    start = dot(gram_ref[...], time_ref[...])
    basis = dot(start, orth_factor(dot(start, start, ((0,), (0,)))))
    time_out_ref[...] = basis * math.sqrt(groups_n)
    wide = dot(spread(groups_n, rank), basis)
    mixer = jnp.where(same_slot(groups_n, rank), dot(wide, wide, ((1,), (1,))), 0.0)
    out_ref[...] = dot(mixer, owned_ref[...])


def mix(gram, time_factor, owned):
    return pl.pallas_call(
        mix_kernel,
        out_shape=(jax.ShapeDtypeStruct(owned.shape, F32), jax.ShapeDtypeStruct(time_factor.shape, F32)),
        name="mix",
    )(gram, time_factor, owned)


def finish_kernel(scale, block_ref, mine_ref, other_ref, out_ref):
    factor = orth_factor(mine_ref[...] + other_ref[...]) * scale
    out_ref[...] = dot(block_ref[...], factor)


def finish(block, mine, other, scale):
    return pl.pallas_call(
        functools.partial(finish_kernel, scale), out_shape=jax.ShapeDtypeStruct(block.shape, F32), name="finish"
    )(block, mine, other)


def row_gram_kernel(block_ref, out_ref):
    block = block_ref[...]
    out_ref[...] = dot(block, block, ((0,), (0,)))


def row_gram(block):
    rank = block.shape[1]
    return pl.pallas_call(row_gram_kernel, out_shape=jax.ShapeDtypeStruct((rank, rank), F32), name="row_gram")(block)


def sum_of_small(part, axes, devices):
    if devices * part.size > 1 << 20:
        return lax.psum(part, axes)
    copies = jnp.broadcast_to(part.reshape(1, -1), (devices, part.size))
    received = lax.all_to_all(copies, axes, split_axis=0, concat_axis=0, tiled=True)
    return jnp.sum(received, axis=0).reshape(part.shape)


def make_on_device(groups_n, reps):
    half_n = groups_n // 2
    halves = [[h * half_n + i for i in range(half_n)] for h in range(2)]
    across = [(i, (i + half_n) % groups_n) for i in range(groups_n)]
    swap = [(0, 1), (1, 0)]

    def all_to_all(value, parts, groups=None):
        shape = value.shape
        value = value.reshape((parts, shape[0] // parts) + shape[1:])
        value = lax.all_to_all(value, "grp", split_axis=0, concat_axis=0, tiled=True, axis_index_groups=groups)
        return value.reshape(shape)

    def on_device(snapshots, row_factor, time_factor):
        rows, cols = snapshots.shape[1:]
        rank = row_factor.shape[1]
        width = cols // reps
        mine = lax.axis_index("rep").astype(jnp.int32).reshape(1)
        partner = 1 - mine
        image = snapshots[0]
        send = project(image, row_factor, partner, width)
        received = lax.ppermute(send, "rep", swap)
        summed = project(image, row_factor, mine, width) + received
        owned = all_to_all(summed, groups_n)
        gram_total = sum_of_small(small_gram(owned, groups_n), ("grp", "rep"), groups_n * reps)
        weights, new_time = mix(gram_total, time_factor, owned)
        weight = all_to_all(weights, groups_n)
        other_weight = lax.ppermute(weight, "rep", swap)
        product = multiply(image, other_weight, partner, multiply(image, weight, mine))
        parts = all_to_all(product, half_n, halves)
        chunk = jnp.sum(parts.reshape(half_n, rows // half_n, rank), axis=0)
        chunk = chunk + lax.ppermute(chunk, "grp", across)
        block = all_to_all(jnp.tile(chunk, (half_n, 1)), half_n, halves)
        gram = row_gram(block)
        new_rows = finish(block, gram, lax.ppermute(gram, "rep", swap), math.sqrt(rows * reps))
        return (new_rows, new_time)

    return on_device


def solution(mesh):
    return jax.shard_map(
        make_on_device(mesh.shape["grp"], mesh.shape["rep"]),
        mesh=mesh,
        in_specs=(P("grp", "rep", None), P("rep", None), P()),
        out_specs=(P("rep", None), P()),
        check_vma=False,
    )
```

```python
import functools
import math

import jax
import jax.numpy as jnp
from jax import lax
from jax.experimental import pallas as pl
from jax.experimental.pallas import tpu as pltpu
from jax.sharding import PartitionSpec as P

STEPS = 8
SMALL = pltpu.CompilerParams(vmem_limit_bytes=16 << 20)
F32 = jnp.float32
BF16 = jnp.bfloat16
TINY = 1e-06


def dot(left, right, contract=((1,), (0,))):
    return lax.dot_general(
        left, right, (contract, ((), ())), precision=lax.Precision.HIGHEST, preferred_element_type=F32
    )


def fastdot(left, right, contract):
    return lax.dot_general(left, right, (contract, ((), ())), preferred_element_type=F32)


def split(value):
    high = value.astype(BF16)
    return high, (value - high.astype(F32)).astype(BF16)


def eye(size):
    return (lax.broadcasted_iota(jnp.int32, (size, size), 0) == lax.broadcasted_iota(jnp.int32, (size, size), 1)).astype(F32)


def orth_factor(gram):
    unit = eye(gram.shape[0])
    total = jnp.sum(gram * unit) + TINY
    squared = gram * (1.0 / total)
    factor = unit * lax.rsqrt(total)
    for step_index in range(STEPS):
        turn = 1.5 * unit - 0.5 * squared
        factor = dot(factor, turn)
        if step_index < STEPS - 1:
            squared = dot(dot(squared, turn), turn)
    return factor


def project_block(image, factor):
    image_high, image_low = split(image)
    factor_high, factor_low = split(factor)
    rank = factor_high.shape[1]
    both = jnp.concatenate([factor_high, factor_low], axis=1)
    wide = fastdot(both, image_high, ((0,), (0,)))
    return wide[:rank] + wide[rank:] + fastdot(factor_high, image_low, ((0,), (0,)))


def first_kernel(which_ref, image_ref, factor_ref, out_ref, held_ref, factor_held_ref, image_sems, factor_sem):
    parts, blocks = image_sems.shape
    rows, width = held_ref.shape[1:]
    block = rows // blocks
    factor_copy = pltpu.make_async_copy(factor_ref, factor_held_ref, factor_sem)
    factor_copy.start()
    copies = []
    for part in range(parts):
        at = pl.multiple_of(which_ref[part] * width, width)
        for i in range(blocks):
            copy = pltpu.make_async_copy(
                image_ref.at[pl.ds(i * block, block), pl.ds(at, width)],
                held_ref.at[part, pl.ds(i * block, block)],
                image_sems.at[part, i],
            )
            copy.start()
            copies.append(copy)
    factor_copy.wait()
    for i in range(blocks):
        copies[i].wait()
        take = pl.ds(i * block, block)
        value = project_block(held_ref[0, take], factor_held_ref[take])
        if i == 0:
            out_ref[...] = value
        else:
            out_ref[...] += value
    for copy in copies[blocks:]:
        copy.wait()


def project_first(image, row_factor, order, width, blocks=4):
    rows = image.shape[0]
    rank = row_factor.shape[1]
    parts = image.shape[1] // width
    return pl.pallas_call(
        first_kernel,
        in_specs=[
            pl.BlockSpec(memory_space=pltpu.SMEM),
            pl.BlockSpec(memory_space=pl.ANY),
            pl.BlockSpec(memory_space=pl.ANY),
        ],
        out_shape=(
            jax.ShapeDtypeStruct((rank, width), F32),
            jax.ShapeDtypeStruct((parts, rows, width), F32),
            jax.ShapeDtypeStruct((rows, rank), F32),
        ),
        scratch_shapes=[pltpu.SemaphoreType.DMA((parts, blocks)), pltpu.SemaphoreType.DMA],
        compiler_params=SMALL,
        name="project_first",
    )(
        order,
        pltpu.with_memory_space_constraint(image, pltpu.HBM),
        pltpu.with_memory_space_constraint(row_factor, pltpu.HBM),
    )


def second_kernel(blocks, held_ref, factor_ref, out_ref):
    block = factor_ref.shape[0] // blocks
    total = None
    for i in range(blocks):
        take = pl.ds(i * block, block)
        value = project_block(held_ref[1, take], factor_ref[take])
        total = value if total is None else total + value
    out_ref[...] = total


def project_second(held, row_factor, blocks=4):
    rows, width = held.shape[1:]
    rank = row_factor.shape[1]
    return pl.pallas_call(
        functools.partial(second_kernel, blocks),
        out_shape=jax.ShapeDtypeStruct((rank, width), F32),
        cost_estimate=pl.CostEstimate(
            flops=6 * rows * width * rank, bytes_accessed=4 * rows * (width + rank), transcendentals=0
        ),
        compiler_params=SMALL,
        name="project_second",
    )(held, row_factor)


def product_kernel(part, blocks, held_ref, weight_ref, *refs):
    out_ref = refs[-1]
    weight_high, weight_low = split(weight_ref[...])
    rank = weight_high.shape[0]
    both = jnp.concatenate([weight_high, weight_low], axis=0)
    block = out_ref.shape[0] // blocks
    for i in range(blocks):
        take = pl.ds(i * block, block)
        image_high, image_low = split(held_ref[part, take])
        wide = fastdot(image_high, both, ((1,), (1,)))
        value = wide[:, :rank] + wide[:, rank:] + fastdot(image_low, weight_high, ((1,), (1,)))
        if len(refs) > 1:
            value = value + refs[0][take]
        out_ref[take] = value


def multiply(held, weight, part, start=None, blocks=4):
    rows, width = held.shape[1:]
    rank = weight.shape[0]
    more = () if start is None else (start,)
    return pl.pallas_call(
        functools.partial(product_kernel, part, blocks),
        out_shape=jax.ShapeDtypeStruct((rows, rank), F32),
        cost_estimate=pl.CostEstimate(
            flops=6 * rows * width * rank, bytes_accessed=4 * rows * (width + rank), transcendentals=0
        ),
        compiler_params=SMALL,
        name="multiply",
    )(held, weight, *more)


def spread(groups_n, rank):
    rows = lax.broadcasted_iota(jnp.int32, (rank, groups_n), 0) // (rank // groups_n)
    return (rows == lax.broadcasted_iota(jnp.int32, (rank, groups_n), 1)).astype(F32)


def same_slot(groups_n, rank):
    per = rank // groups_n
    left = lax.broadcasted_iota(jnp.int32, (rank, rank), 0) % per
    right = lax.broadcasted_iota(jnp.int32, (rank, rank), 1) % per
    return left == right


def cell_rows(groups_n, cells):
    rows = lax.broadcasted_iota(jnp.int32, (groups_n, cells), 0)
    return (rows == lax.broadcasted_iota(jnp.int32, (groups_n, cells), 1) // groups_n).astype(F32)


def cell_columns(groups_n, cells):
    columns = lax.broadcasted_iota(jnp.int32, (groups_n, cells), 0)
    return (columns == lax.broadcasted_iota(jnp.int32, (groups_n, cells), 1) % groups_n).astype(F32)


def gram_of(owned, groups_n):
    rank = owned.shape[0]
    full = jnp.where(same_slot(groups_n, rank), dot(owned, owned, ((1,), (1,))), 0.0)
    fold = spread(groups_n, rank)
    return dot(dot(fold, full, ((0,), (0,))), fold)


def gram_kernel(groups_n, owned_ref, out_ref):
    gram = gram_of(owned_ref[...], groups_n)
    if len(out_ref.shape) == 2:
        out_ref[...] = gram
    else:
        cells = out_ref.shape[2]
        flat = jnp.sum(cell_rows(groups_n, cells) * dot(gram, cell_columns(groups_n, cells)), axis=0, keepdims=True)
        out_ref[...] = jnp.broadcast_to(flat[None], out_ref.shape)


def small_gram(owned, groups_n, shape):
    return pl.pallas_call(
        functools.partial(gram_kernel, groups_n),
        out_shape=jax.ShapeDtypeStruct(shape, F32),
        compiler_params=SMALL,
        name="small_gram",
    )(owned)


def mix_kernel(groups_n, gram_ref, time_ref, owned_ref, out_ref, time_out_ref):
    rank = owned_ref.shape[0]
    if len(gram_ref.shape) == 2:
        gram = gram_ref[...]
    else:
        cells = gram_ref.shape[2]
        flat = jnp.sum(gram_ref[...], axis=0)
        gram = dot(cell_rows(groups_n, cells) * flat, cell_columns(groups_n, cells), ((1,), (1,)))
    start = dot(gram, time_ref[...], ((1,), (1,)))
    basis = dot(start, orth_factor(dot(start, start, ((0,), (0,)))))
    time_out_ref[...] = basis * math.sqrt(groups_n)
    wide = dot(spread(groups_n, rank), basis)
    mixer = jnp.where(same_slot(groups_n, rank), dot(wide, wide, ((1,), (1,))), 0.0)
    out_ref[...] = dot(mixer, owned_ref[...])


def mix(gram, time_factor, owned, groups_n):
    return pl.pallas_call(
        functools.partial(mix_kernel, groups_n),
        out_shape=(jax.ShapeDtypeStruct(owned.shape, F32), jax.ShapeDtypeStruct(time_factor.shape, F32)),
        compiler_params=SMALL,
        name="mix",
    )(gram, time_factor.T, owned)


def finish_kernel(scale, block_ref, mine_ref, other_ref, out_ref):
    factor = orth_factor(mine_ref[...] + other_ref[...]) * scale
    out_ref[...] = dot(block_ref[...], factor)


def finish(block, mine, other, scale):
    return pl.pallas_call(
        functools.partial(finish_kernel, scale), out_shape=jax.ShapeDtypeStruct(block.shape, F32), compiler_params=SMALL, name="finish"
    )(block, mine, other)


def row_gram_kernel(block_ref, out_ref):
    block = block_ref[...]
    out_ref[...] = dot(block, block, ((0,), (0,)))


def row_gram(block):
    rank = block.shape[1]
    return pl.pallas_call(row_gram_kernel, out_shape=jax.ShapeDtypeStruct((rank, rank), F32), compiler_params=SMALL, name="row_gram")(block)


def make_on_device(groups_n, reps):
    half_n = groups_n // 2
    halves = [[h * half_n + i for i in range(half_n)] for h in range(2)]
    across = [(i, (i + half_n) % groups_n) for i in range(groups_n)]
    swap = [(0, 1), (1, 0)]

    def all_to_all(value, parts, groups=None):
        shape = value.shape
        value = value.reshape((parts, shape[0] // parts) + shape[1:])
        value = lax.all_to_all(value, "grp", split_axis=0, concat_axis=0, tiled=True, axis_index_groups=groups)
        return value.reshape(shape)

    def on_device(snapshots, row_factor, time_factor):
        rows, cols = snapshots.shape[1:]
        rank = row_factor.shape[1]
        width = cols // reps
        mine = lax.axis_index("rep").astype(jnp.int32)
        order = jnp.stack([1 - mine, mine])
        send, held, factor = project_first(snapshots[0], row_factor, order, width)
        received = lax.ppermute(send, "rep", swap)
        summed = project_second(held, factor) + received
        owned = all_to_all(summed, groups_n)
        devices = groups_n * reps
        if devices * groups_n * groups_n <= 1 << 20:
            grams = lax.all_to_all(
                small_gram(owned, groups_n, (devices, 1, groups_n * groups_n)),
                ("grp", "rep"),
                split_axis=0,
                concat_axis=0,
                tiled=True,
            )
        else:
            grams = lax.psum(small_gram(owned, groups_n, (groups_n, groups_n)), ("grp", "rep"))
        weights, new_time = mix(grams, time_factor, owned, groups_n)
        weight = all_to_all(weights, groups_n)
        other_weight = lax.ppermute(weight, "rep", swap)
        product = multiply(held, other_weight, 0, multiply(held, weight, 1))
        parts = all_to_all(product, half_n, halves)
        chunk = jnp.sum(parts.reshape(half_n, rows // half_n, rank), axis=0)
        chunk = chunk + lax.ppermute(chunk, "grp", across)
        block = all_to_all(jnp.tile(chunk, (half_n, 1)), half_n, halves)
        gram = row_gram(block)
        new_rows = finish(block, gram, lax.ppermute(gram, "rep", swap), math.sqrt(rows * reps))
        return (new_rows, new_time)

    return on_device


def solution(mesh):
    return jax.shard_map(
        make_on_device(mesh.shape["grp"], mesh.shape["rep"]),
        mesh=mesh,
        in_specs=(P("grp", "rep", None), P("rep", None), P()),
        out_specs=(P("rep", None), P()),
        check_vma=False,
    )
```

```python
import functools
import math

import jax
import jax.numpy as jnp
from jax import lax
from jax.experimental import pallas as pl
from jax.experimental.pallas import tpu as pltpu
from jax.sharding import PartitionSpec as P

STEPS = 8
SMALL = pltpu.CompilerParams(vmem_limit_bytes=16 << 20)
F32 = jnp.float32
BF16 = jnp.bfloat16
TINY = 1e-06


def dot(left, right, contract=((1,), (0,))):
    return lax.dot_general(
        left, right, (contract, ((), ())), precision=lax.Precision.HIGHEST, preferred_element_type=F32
    )


def fastdot(left, right, contract):
    return lax.dot_general(left, right, (contract, ((), ())), preferred_element_type=F32)


def split(value):
    high = value.astype(BF16)
    return high, (value - high.astype(F32)).astype(BF16)


def eye(size):
    return (lax.broadcasted_iota(jnp.int32, (size, size), 0) == lax.broadcasted_iota(jnp.int32, (size, size), 1)).astype(F32)


def split3(value):
    high = value.astype(BF16)
    rest = value - high.astype(F32)
    middle = rest.astype(BF16)
    return high, middle, (rest - middle.astype(F32)).astype(BF16)


def left6(value):
    high, middle, low = split3(value)
    return jnp.concatenate([high, high, middle, high, middle, low], axis=1)


def right6(value):
    high, middle, low = split3(value)
    return jnp.concatenate([high, middle, high, low, middle, high], axis=0)


def times(right):
    size = right.shape[0]
    if size <= 16:
        rows = [right[k : k + 1, :] for k in range(size)]

        def apply(left):
            terms = [left[:, k : k + 1] * rows[k] for k in range(size)]
            while len(terms) > 1:
                terms = [sum(terms[i : i + 2]) for i in range(0, len(terms), 2)]
            return terms[0]

        return apply
    if size % 128 == 0:
        stacked = right6(right)
        return lambda left: fastdot(left6(left), stacked, ((1,), (0,)))
    return lambda left: dot(left, right)


def orth_factor(gram):
    unit = eye(gram.shape[0])
    total = jnp.sum(gram * unit) + TINY
    squared = gram * (1.0 / total)
    factor = unit * lax.rsqrt(total)
    for step_index in range(STEPS):
        turn = 1.5 * unit - 0.5 * squared
        by_turn = times(turn)
        factor = by_turn(factor) if step_index else factor[:1, :1] * turn
        if step_index < STEPS - 1:
            squared = by_turn(by_turn(squared))
    return factor


def halves_of(value):
    high, low = split(value)
    return jnp.concatenate([high, low], axis=1)


def project_block(image_high, image_low, factor_both):
    rank = factor_both.shape[1] // 2
    wide = fastdot(factor_both, image_high, ((0,), (0,)))
    return wide[:rank] + wide[rank:] + fastdot(factor_both[:, :rank], image_low, ((0,), (0,)))


def first_kernel(
    image_ref, factor_ref, out_ref, high_ref, low_ref, later_ref, both_ref, now_ref, fetched_ref, image_sems, factor_sem
):
    parts, blocks = image_sems.shape
    rows, width = now_ref.shape
    block = rows // blocks
    me = lax.axis_index("rep")
    factor_copy = pltpu.make_async_copy(factor_ref, fetched_ref, factor_sem)
    factor_copy.start()
    copies = []
    for part, held_ref in enumerate((now_ref, later_ref)):
        at = pl.multiple_of(lax.rem(me + 1 + part, parts) * width, width)
        for i in range(blocks):
            take = pl.ds(i * block, block)
            copy = pltpu.make_async_copy(image_ref.at[take, pl.ds(at, width)], held_ref.at[take], image_sems.at[part, i])
            copies.append(copy)
    for copy in copies[:blocks]:
        copy.start()
    factor_copy.wait()
    both_ref[...] = halves_of(fetched_ref[...])
    for i in range(blocks):
        copies[i].wait()
        copies[blocks + i].start()
        take = pl.ds(i * block, block)
        high, low = split(now_ref[take])
        high_ref[take] = high
        low_ref[take] = low
        value = project_block(high, low, both_ref[take])
        if i == 0:
            out_ref[...] = value
        else:
            out_ref[...] += value
    for copy in copies[blocks:]:
        copy.wait()


def project_first(image, row_factor, width, blocks=4):
    rows = image.shape[0]
    rank = row_factor.shape[1]
    parts = image.shape[1] // width
    return pl.pallas_call(
        first_kernel,
        in_specs=[pl.BlockSpec(memory_space=pl.ANY), pl.BlockSpec(memory_space=pl.ANY)],
        out_shape=(
            jax.ShapeDtypeStruct((rank, width), F32),
            jax.ShapeDtypeStruct((rows, width), BF16),
            jax.ShapeDtypeStruct((rows, width), BF16),
            jax.ShapeDtypeStruct((rows, width), F32),
            jax.ShapeDtypeStruct((rows, 2 * rank), BF16),
        ),
        scratch_shapes=[
            pltpu.VMEM((rows, width), F32),
            pltpu.VMEM((rows, rank), F32),
            pltpu.SemaphoreType.DMA((parts, blocks)),
            pltpu.SemaphoreType.DMA,
        ],
        compiler_params=SMALL,
        name="project_first",
    )(
        pltpu.with_memory_space_constraint(image, pltpu.HBM),
        pltpu.with_memory_space_constraint(row_factor, pltpu.HBM),
    )


def second_kernel(blocks, image_ref, both_ref, out_ref, high_ref, low_ref):
    block = image_ref.shape[0] // blocks
    total = None
    for i in range(blocks):
        take = pl.ds(i * block, block)
        high, low = split(image_ref[take])
        high_ref[take] = high
        low_ref[take] = low
        value = project_block(high, low, both_ref[take])
        total = value if total is None else total + value
    out_ref[...] = total


def project_second(image, both, blocks=4):
    rows, width = image.shape
    rank = both.shape[1] // 2
    return pl.pallas_call(
        functools.partial(second_kernel, blocks),
        out_shape=(
            jax.ShapeDtypeStruct((rank, width), F32),
            jax.ShapeDtypeStruct((rows, width), BF16),
            jax.ShapeDtypeStruct((rows, width), BF16),
        ),
        cost_estimate=pl.CostEstimate(
            flops=6 * rows * width * rank, bytes_accessed=4 * rows * (width + rank), transcendentals=0
        ),
        compiler_params=SMALL,
        name="project_second",
    )(image, both)


def product_kernel(blocks, high_ref, low_ref, weight_ref, *refs):
    out_ref = refs[-1]
    weight_high, weight_low = split(weight_ref[...])
    rank = weight_high.shape[0]
    both = jnp.concatenate([weight_high, weight_low], axis=0)
    block = out_ref.shape[0] // blocks
    for i in range(blocks):
        take = pl.ds(i * block, block)
        wide = fastdot(high_ref[take], both, ((1,), (1,)))
        value = wide[:, :rank] + wide[:, rank:] + fastdot(low_ref[take], weight_high, ((1,), (1,)))
        if len(refs) > 1:
            value = value + refs[0][take]
        out_ref[take] = value


def multiply(high, low, weight, start=None, blocks=4):
    rows, width = high.shape
    rank = weight.shape[0]
    more = () if start is None else (start,)
    return pl.pallas_call(
        functools.partial(product_kernel, blocks),
        out_shape=jax.ShapeDtypeStruct((rows, rank), F32),
        cost_estimate=pl.CostEstimate(
            flops=6 * rows * width * rank, bytes_accessed=4 * rows * (width + rank), transcendentals=0
        ),
        compiler_params=SMALL,
        name="multiply",
    )(high, low, weight, *more)


def cells(rows, count, row_of, cell_of):
    row = row_of(lax.broadcasted_iota(jnp.int32, (rows, count), 0))
    return (row == cell_of(lax.broadcasted_iota(jnp.int32, (rows, count), 1))).astype(F32)


def spread(groups_n, rank):
    per = rank // groups_n
    return cells(rank, groups_n, lambda row: row // per, lambda cell: cell)


def same_slot(groups_n, rank):
    per = rank // groups_n
    return cells(rank, rank, lambda row: row % per, lambda cell: cell % per) > 0.5


def gram_kernel(groups_n, owned_ref, out_ref):
    owned = owned_ref[...]
    rank = owned.shape[0]
    per = rank // groups_n
    full = jnp.where(same_slot(groups_n, rank), dot(owned, owned, ((1,), (1,))), 0.0)
    if len(out_ref.shape) == 2:
        fold = spread(groups_n, rank)
        out_ref[...] = dot(dot(fold, full, ((0,), (0,))), fold)
    else:
        count = out_ref.shape[2]
        columns = cells(rank, count, lambda row: row // per, lambda cell: cell % groups_n).astype(BF16)
        folded = fastdot(
            jnp.concatenate(split3(full), axis=1), jnp.concatenate([columns, columns, columns], axis=0), ((1,), (0,))
        )
        rows = cells(rank, count, lambda row: row // per, lambda cell: cell // groups_n)
        flat = jnp.sum(rows * folded, axis=0, keepdims=True)
        out_ref[...] = jnp.broadcast_to(flat[None], out_ref.shape)


def small_gram(owned, groups_n, shape):
    return pl.pallas_call(
        functools.partial(gram_kernel, groups_n),
        out_shape=jax.ShapeDtypeStruct(shape, F32),
        compiler_params=SMALL,
        name="small_gram",
    )(owned)


def mix_kernel(groups_n, gram_ref, time_ref, owned_ref, out_ref, time_out_ref):
    rank = owned_ref.shape[0]
    per = rank // groups_n
    if len(gram_ref.shape) == 2:
        fold = spread(groups_n, rank)
        start = dot(fold, dot(gram_ref[...], time_ref[...], ((1,), (1,))))
        turned = dot(dot(time_ref[...], gram_ref[...], ((1,), (1,))), fold, ((1,), (1,)))
    else:
        count = gram_ref.shape[2]
        flat = jnp.sum(gram_ref[...], axis=0)
        rows = cells(rank, count, lambda row: row // per, lambda cell: cell // groups_n) * flat
        columns = dot(time_ref[...], cells(groups_n, count, lambda row: row, lambda cell: cell % groups_n))
        start = dot(rows, columns, ((1,), (1,)))
        turned = dot(columns, rows, ((1,), (1,)))
    basis = dot(start, orth_factor(dot(turned, start) * (1.0 / per)))
    mixer = jnp.where(same_slot(groups_n, rank), dot(basis, basis, ((1,), (1,))), 0.0)
    mixer_high, mixer_low = split(mixer)
    owned_high, owned_low = split(owned_ref[...])
    out_ref[...] = fastdot(
        jnp.concatenate([mixer_high, mixer_low, mixer_high], axis=1),
        jnp.concatenate([owned_high, owned_high, owned_low], axis=0),
        ((1,), (0,)),
    )
    one_of_each = cells(groups_n, rank, lambda row: row * per, lambda cell: cell)
    time_out_ref[...] = dot(one_of_each, basis) * math.sqrt(groups_n)


def mix(gram, time_factor, owned, groups_n):
    return pl.pallas_call(
        functools.partial(mix_kernel, groups_n),
        out_shape=(jax.ShapeDtypeStruct(owned.shape, F32), jax.ShapeDtypeStruct(time_factor.shape, F32)),
        compiler_params=SMALL,
        name="mix",
    )(gram, time_factor.T, owned)


def finish_kernel(scale, blocks, block_ref, mine_ref, other_ref, out_ref, made_ref, sems):
    rows = block_ref.shape[0] // blocks
    high, low = split(block_ref[...])
    left = jnp.concatenate([high, low, high], axis=1)
    factor_high, factor_low = split(orth_factor(mine_ref[...] + other_ref[...]) * scale)
    right = jnp.concatenate([factor_high, factor_high, factor_low], axis=0)
    copies = []
    for i in range(blocks):
        take = pl.ds(i * rows, rows)
        made_ref[take] = fastdot(left[i * rows : (i + 1) * rows], right, ((1,), (0,)))
        copies.append(pltpu.make_async_copy(made_ref.at[take], out_ref.at[take], sems.at[i]))
        copies[-1].start()
    for copy in copies:
        copy.wait()


def finish(block, mine, other, scale, blocks=4):
    return pl.pallas_call(
        functools.partial(finish_kernel, scale, blocks),
        out_shape=jax.ShapeDtypeStruct(block.shape, F32),
        out_specs=pl.BlockSpec(memory_space=pl.ANY),
        scratch_shapes=[pltpu.VMEM(block.shape, F32), pltpu.SemaphoreType.DMA((blocks,))],
        compiler_params=SMALL,
        name="finish",
    )(block, mine, other)


def row_gram_kernel(block_ref, out_ref):
    block = block_ref[...]
    out_ref[...] = dot(block, block, ((0,), (0,)))


def row_gram(block):
    rank = block.shape[1]
    return pl.pallas_call(row_gram_kernel, out_shape=jax.ShapeDtypeStruct((rank, rank), F32), compiler_params=SMALL, name="row_gram")(block)


def make_on_device(groups_n, reps):
    half_n = groups_n // 2
    halves = [[h * half_n + i for i in range(half_n)] for h in range(2)]
    across = [(i, (i + half_n) % groups_n) for i in range(groups_n)]
    swap = [(0, 1), (1, 0)]

    def all_to_all(value, parts, groups=None):
        shape = value.shape
        value = value.reshape((parts, shape[0] // parts) + shape[1:])
        value = lax.all_to_all(value, "grp", split_axis=0, concat_axis=0, tiled=True, axis_index_groups=groups)
        return value.reshape(shape)

    def on_device(snapshots, row_factor, time_factor):
        rows, cols = snapshots.shape[1:]
        rank = row_factor.shape[1]
        width = cols // reps
        send, far_high, far_low, near, both = project_first(snapshots[0], row_factor, width)
        received = lax.ppermute(send, "rep", swap)
        summed, near_high, near_low = project_second(near, both)
        summed = summed + received
        owned = all_to_all(summed, groups_n)
        devices = groups_n * reps
        if devices * groups_n * groups_n <= 1 << 20:
            grams = lax.all_to_all(
                small_gram(owned, groups_n, (devices, 1, groups_n * groups_n)),
                ("grp", "rep"),
                split_axis=0,
                concat_axis=0,
                tiled=True,
            )
        else:
            grams = lax.psum(small_gram(owned, groups_n, (groups_n, groups_n)), ("grp", "rep"))
        weights, new_time = mix(grams, time_factor, owned, groups_n)
        weight = all_to_all(weights, groups_n)
        other_weight = lax.ppermute(weight, "rep", swap)
        product = multiply(far_high, far_low, other_weight, multiply(near_high, near_low, weight))
        parts = all_to_all(product, half_n, halves)
        chunk = jnp.sum(parts.reshape(half_n, rows // half_n, rank), axis=0)
        chunk = chunk + lax.ppermute(chunk, "grp", across)
        block = all_to_all(jnp.tile(chunk, (half_n, 1)), half_n, halves)
        gram = row_gram(block)
        new_rows = finish(block, gram, lax.ppermute(gram, "rep", swap), math.sqrt(rows * reps))
        return (new_rows, new_time)

    return on_device


def solution(mesh):
    return jax.shard_map(
        make_on_device(mesh.shape["grp"], mesh.shape["rep"]),
        mesh=mesh,
        in_specs=(P("grp", "rep", None), P("rep", None), P()),
        out_specs=(P("rep", None), P()),
        check_vma=False,
    )
```

```python
import functools
import math

import jax
import jax.numpy as jnp
from jax import lax
from jax.experimental import pallas as pl
from jax.experimental.pallas import tpu as pltpu
from jax.sharding import PartitionSpec as P

STEPS = 8
SMALL = pltpu.CompilerParams(vmem_limit_bytes=16 << 20)
F32 = jnp.float32
BF16 = jnp.bfloat16
TINY = 1e-06


def dot(left, right, contract=((1,), (0,))):
    return lax.dot_general(
        left, right, (contract, ((), ())), precision=lax.Precision.HIGHEST, preferred_element_type=F32
    )


def fastdot(left, right, contract):
    return lax.dot_general(left, right, (contract, ((), ())), preferred_element_type=F32)


def split(value):
    high = value.astype(BF16)
    return high, (value - high.astype(F32)).astype(BF16)


def eye(size):
    return (lax.broadcasted_iota(jnp.int32, (size, size), 0) == lax.broadcasted_iota(jnp.int32, (size, size), 1)).astype(F32)


def split3(value):
    high = value.astype(BF16)
    rest = value - high.astype(F32)
    middle = rest.astype(BF16)
    return high, middle, (rest - middle.astype(F32)).astype(BF16)


def tree_sum(terms):
    while len(terms) > 1:
        terms = [sum(terms[i : i + 2]) for i in range(0, len(terms), 2)]
    return terms[0]


def small_step(squared, factor, unit):
    size = unit.shape[0]
    columns = [jnp.broadcast_to(squared[:, k : k + 1], unit.shape) for k in range(size)]
    turn = 1.5 * unit - 0.5 * squared
    turn_columns = [1.5 * unit[:, k : k + 1] - 0.5 * columns[k] for k in range(size)]
    turn_squared = tree_sum([turn_columns[k] * turn[k : k + 1] for k in range(size)])
    factor = tree_sum([turn_columns[k] * factor[k : k + 1] for k in range(size)])
    return tree_sum([columns[k] * turn_squared[k : k + 1] for k in range(size)]), factor


def step(squared, factor, unit):
    if unit.shape[0] <= 16:
        return small_step(squared, factor, unit)
    turn = 1.5 * unit - 0.5 * squared
    if unit.shape[0] % 128:
        return dot(dot(squared, turn), turn), dot(factor, turn)
    high, low = split(squared)
    stacked = jnp.concatenate([high, low, high], axis=0)

    def by_squared(left):
        left_high, left_low = split(left)
        return fastdot(jnp.concatenate([left_high, left_high, left_low], axis=1), stacked, ((1,), (0,)))

    rank = unit.shape[0]
    both = by_squared(jnp.concatenate([squared, factor], axis=0))
    turn = 2.25 * unit - 1.5 * squared + 0.25 * both[:rank]
    return by_squared(turn), 1.5 * factor - 0.5 * both[rank:]


def orth_factor(gram):
    unit = eye(gram.shape[0])
    total = jnp.sum(gram * unit) + TINY
    squared = gram * (1.0 / total)
    factor = unit * lax.rsqrt(total)
    for step_index in range(STEPS):
        squared, factor = step(squared, factor, unit)
    return factor


def halves_of(value):
    high, low = split(value)
    return jnp.concatenate([high, low], axis=1)


def project_block(image_high, image_low, factor_both):
    rank = factor_both.shape[1] // 2
    wide = fastdot(factor_both, image_high, ((0,), (0,)))
    return wide[:rank] + wide[rank:] + fastdot(factor_both[:, :rank], image_low, ((0,), (0,)))


def first_kernel(
    image_ref, factor_ref, out_ref, high_ref, low_ref, later_ref, both_ref, now_ref, fetched_ref, image_sems, factor_sem
):
    parts, blocks = image_sems.shape
    rows, width = now_ref.shape
    block = rows // blocks
    me = lax.axis_index("rep")
    factor_copy = pltpu.make_async_copy(factor_ref, fetched_ref, factor_sem)
    factor_copy.start()
    copies = []
    for part, held_ref in enumerate((now_ref, later_ref)):
        at = pl.multiple_of(lax.rem(me + 1 + part, parts) * width, width)
        for i in range(blocks):
            take = pl.ds(i * block, block)
            copy = pltpu.make_async_copy(image_ref.at[take, pl.ds(at, width)], held_ref.at[take], image_sems.at[part, i])
            copies.append(copy)
    for copy in copies[:blocks]:
        copy.start()
    factor_copy.wait()
    both_ref[...] = halves_of(fetched_ref[...])
    for i in range(blocks):
        copies[i].wait()
        copies[blocks + i].start()
        take = pl.ds(i * block, block)
        high, low = split(now_ref[take])
        high_ref[take] = high
        low_ref[take] = low
        value = project_block(high, low, both_ref[take])
        if i == 0:
            out_ref[...] = value
        else:
            out_ref[...] += value
    for copy in copies[blocks:]:
        copy.wait()


def project_first(image, row_factor, width, blocks=4):
    rows = image.shape[0]
    rank = row_factor.shape[1]
    parts = image.shape[1] // width
    return pl.pallas_call(
        first_kernel,
        in_specs=[pl.BlockSpec(memory_space=pl.ANY), pl.BlockSpec(memory_space=pl.ANY)],
        out_shape=(
            jax.ShapeDtypeStruct((rank, width), F32),
            jax.ShapeDtypeStruct((rows, width), BF16),
            jax.ShapeDtypeStruct((rows, width), BF16),
            jax.ShapeDtypeStruct((rows, width), F32),
            jax.ShapeDtypeStruct((rows, 2 * rank), BF16),
        ),
        scratch_shapes=[
            pltpu.VMEM((rows, width), F32),
            pltpu.VMEM((rows, rank), F32),
            pltpu.SemaphoreType.DMA((parts, blocks)),
            pltpu.SemaphoreType.DMA,
        ],
        compiler_params=SMALL,
        name="project_first",
    )(
        pltpu.with_memory_space_constraint(image, pltpu.HBM),
        pltpu.with_memory_space_constraint(row_factor, pltpu.HBM),
    )


def second_kernel(blocks, image_ref, both_ref, out_ref, high_ref, low_ref):
    block = image_ref.shape[0] // blocks
    total = None
    for i in range(blocks):
        take = pl.ds(i * block, block)
        high, low = split(image_ref[take])
        high_ref[take] = high
        low_ref[take] = low
        value = project_block(high, low, both_ref[take])
        total = value if total is None else total + value
    out_ref[...] = total


def project_second(image, both, blocks=4):
    rows, width = image.shape
    rank = both.shape[1] // 2
    return pl.pallas_call(
        functools.partial(second_kernel, blocks),
        out_shape=(
            jax.ShapeDtypeStruct((rank, width), F32),
            jax.ShapeDtypeStruct((rows, width), BF16),
            jax.ShapeDtypeStruct((rows, width), BF16),
        ),
        cost_estimate=pl.CostEstimate(
            flops=6 * rows * width * rank, bytes_accessed=4 * rows * (width + rank), transcendentals=0
        ),
        compiler_params=SMALL,
        name="project_second",
    )(image, both)


def product_kernel(blocks, high_ref, low_ref, weight_ref, *refs):
    out_ref = refs[-1]
    weight_high, weight_low = split(weight_ref[...])
    rank = weight_high.shape[0]
    both = jnp.concatenate([weight_high, weight_low], axis=0)
    block = out_ref.shape[0] // blocks
    for i in range(blocks):
        take = pl.ds(i * block, block)
        wide = fastdot(high_ref[take], both, ((1,), (1,)))
        value = wide[:, :rank] + wide[:, rank:] + fastdot(low_ref[take], weight_high, ((1,), (1,)))
        if len(refs) > 1:
            value = value + refs[0][take]
        out_ref[take] = value


def multiply(high, low, weight, start=None, blocks=4):
    rows, width = high.shape
    rank = weight.shape[0]
    more = () if start is None else (start,)
    return pl.pallas_call(
        functools.partial(product_kernel, blocks),
        out_shape=jax.ShapeDtypeStruct((rows, rank), F32),
        cost_estimate=pl.CostEstimate(
            flops=6 * rows * width * rank, bytes_accessed=4 * rows * (width + rank), transcendentals=0
        ),
        compiler_params=SMALL,
        name="multiply",
    )(high, low, weight, *more)


def cells(rows, count, row_of, cell_of):
    row = row_of(lax.broadcasted_iota(jnp.int32, (rows, count), 0))
    return (row == cell_of(lax.broadcasted_iota(jnp.int32, (rows, count), 1))).astype(F32)


def spread(groups_n, rank):
    per = rank // groups_n
    return cells(rank, groups_n, lambda row: row // per, lambda cell: cell)


def same_slot(groups_n, rank):
    per = rank // groups_n
    return cells(rank, rank, lambda row: row % per, lambda cell: cell % per) > 0.5


def gram_kernel(groups_n, owned_ref, out_ref):
    owned = owned_ref[...]
    rank = owned.shape[0]
    per = rank // groups_n
    full = jnp.where(same_slot(groups_n, rank), dot(owned, owned, ((1,), (1,))), 0.0)
    if len(out_ref.shape) == 2:
        fold = spread(groups_n, rank)
        out_ref[...] = dot(dot(fold, full, ((0,), (0,))), fold)
    else:
        count = out_ref.shape[2]
        columns = cells(rank, count, lambda row: row // per, lambda cell: cell % groups_n).astype(BF16)
        folded = fastdot(
            jnp.concatenate(split3(full), axis=1), jnp.concatenate([columns, columns, columns], axis=0), ((1,), (0,))
        )
        rows = cells(rank, count, lambda row: row // per, lambda cell: cell // groups_n)
        flat = jnp.sum(rows * folded, axis=0, keepdims=True)
        out_ref[...] = jnp.broadcast_to(flat[None], out_ref.shape)


def small_gram(owned, groups_n, shape):
    return pl.pallas_call(
        functools.partial(gram_kernel, groups_n),
        out_shape=jax.ShapeDtypeStruct(shape, F32),
        compiler_params=SMALL,
        name="small_gram",
    )(owned)


def mix_kernel(groups_n, gram_ref, time_ref, owned_ref, out_ref, time_out_ref):
    rank = owned_ref.shape[0]
    per = rank // groups_n
    if len(gram_ref.shape) == 2:
        fold = spread(groups_n, rank)
        start = dot(fold, dot(gram_ref[...], time_ref[...], ((1,), (1,))))
        turned = dot(dot(time_ref[...], gram_ref[...], ((1,), (1,))), fold, ((1,), (1,)))
    else:
        count = gram_ref.shape[2]
        flat = jnp.sum(gram_ref[...], axis=0)
        rows = cells(rank, count, lambda row: row // per, lambda cell: cell // groups_n) * flat
        columns = dot(time_ref[...], cells(groups_n, count, lambda row: row, lambda cell: cell % groups_n))
        start = dot(rows, columns, ((1,), (1,)))
        turned = dot(columns, rows, ((1,), (1,)))
    basis = dot(start, orth_factor(dot(turned, start) * (1.0 / per)))
    mixer = jnp.where(same_slot(groups_n, rank), dot(basis, basis, ((1,), (1,))), 0.0)
    mixer_high, mixer_low = split(mixer)
    owned_high, owned_low = split(owned_ref[...])
    out_ref[...] = fastdot(
        jnp.concatenate([mixer_high, mixer_low, mixer_high], axis=1),
        jnp.concatenate([owned_high, owned_high, owned_low], axis=0),
        ((1,), (0,)),
    )
    one_of_each = cells(groups_n, rank, lambda row: row * per, lambda cell: cell)
    time_out_ref[...] = dot(one_of_each, basis) * math.sqrt(groups_n)


def mix(gram, time_factor, owned, groups_n):
    return pl.pallas_call(
        functools.partial(mix_kernel, groups_n),
        out_shape=(jax.ShapeDtypeStruct(owned.shape, F32), jax.ShapeDtypeStruct(time_factor.shape, F32)),
        compiler_params=SMALL,
        name="mix",
    )(gram, time_factor.T, owned)


def finish_kernel(scale, blocks, block_ref, mine_ref, other_ref, out_ref, made_ref, sems):
    rows = block_ref.shape[0] // blocks
    high, low = split(block_ref[...])
    left = jnp.concatenate([high, low, high], axis=1)
    factor_high, factor_low = split(orth_factor(mine_ref[...] + other_ref[...]) * scale)
    right = jnp.concatenate([factor_high, factor_high, factor_low], axis=0)
    copies = []
    for i in range(blocks):
        take = pl.ds(i * rows, rows)
        made_ref[take] = fastdot(left[i * rows : (i + 1) * rows], right, ((1,), (0,)))
        copies.append(pltpu.make_async_copy(made_ref.at[take], out_ref.at[take], sems.at[i]))
        copies[-1].start()
    for copy in copies:
        copy.wait()


def finish(block, mine, other, scale, blocks=4):
    return pl.pallas_call(
        functools.partial(finish_kernel, scale, blocks),
        out_shape=jax.ShapeDtypeStruct(block.shape, F32),
        out_specs=pl.BlockSpec(memory_space=pl.ANY),
        scratch_shapes=[pltpu.VMEM(block.shape, F32), pltpu.SemaphoreType.DMA((blocks,))],
        compiler_params=SMALL,
        name="finish",
    )(block, mine, other)


def row_gram_kernel(block_ref, out_ref):
    block = block_ref[...]
    out_ref[...] = dot(block, block, ((0,), (0,)))


def row_gram(block):
    rank = block.shape[1]
    return pl.pallas_call(row_gram_kernel, out_shape=jax.ShapeDtypeStruct((rank, rank), F32), compiler_params=SMALL, name="row_gram")(block)


def make_on_device(groups_n, reps):
    half_n = groups_n // 2
    halves = [[h * half_n + i for i in range(half_n)] for h in range(2)]
    across = [(i, (i + half_n) % groups_n) for i in range(groups_n)]
    swap = [(0, 1), (1, 0)]

    def all_to_all(value, parts, groups=None):
        shape = value.shape
        value = value.reshape((parts, shape[0] // parts) + shape[1:])
        value = lax.all_to_all(value, "grp", split_axis=0, concat_axis=0, tiled=True, axis_index_groups=groups)
        return value.reshape(shape)

    def on_device(snapshots, row_factor, time_factor):
        rows, cols = snapshots.shape[1:]
        rank = row_factor.shape[1]
        width = cols // reps
        send, far_high, far_low, near, both = project_first(snapshots[0], row_factor, width)
        received = lax.ppermute(send, "rep", swap)
        summed, near_high, near_low = project_second(near, both)
        summed = summed + received
        owned = all_to_all(summed, groups_n)
        devices = groups_n * reps
        if devices * groups_n * groups_n <= 1 << 20:
            grams = lax.all_to_all(
                small_gram(owned, groups_n, (devices, 1, groups_n * groups_n)),
                ("grp", "rep"),
                split_axis=0,
                concat_axis=0,
                tiled=True,
            )
        else:
            grams = lax.psum(small_gram(owned, groups_n, (groups_n, groups_n)), ("grp", "rep"))
        weights, new_time = mix(grams, time_factor, owned, groups_n)
        weight = all_to_all(weights, groups_n)
        other_weight = lax.ppermute(weight, "rep", swap)
        product = multiply(far_high, far_low, other_weight, multiply(near_high, near_low, weight))
        parts = all_to_all(product, half_n, halves)
        chunk = jnp.sum(parts.reshape(half_n, rows // half_n, rank), axis=0)
        chunk = chunk + lax.ppermute(chunk, "grp", across)
        block = all_to_all(jnp.tile(chunk, (half_n, 1)), half_n, halves)
        gram = row_gram(block)
        new_rows = finish(block, gram, lax.ppermute(gram, "rep", swap), math.sqrt(rows * reps))
        return (new_rows, new_time)

    return on_device


def solution(mesh):
    return jax.shard_map(
        make_on_device(mesh.shape["grp"], mesh.shape["rep"]),
        mesh=mesh,
        in_specs=(P("grp", "rep", None), P("rep", None), P()),
        out_specs=(P("rep", None), P()),
        check_vma=False,
    )
```

```python
import functools
import math

import jax
import jax.numpy as jnp
from jax import lax
from jax.experimental import pallas as pl
from jax.experimental.pallas import tpu as pltpu
from jax.sharding import PartitionSpec as P

STEPS = 8
SMALL = pltpu.CompilerParams(vmem_limit_bytes=16 << 20)
F32 = jnp.float32
BF16 = jnp.bfloat16
TINY = 1e-06


def dot(left, right, contract=((1,), (0,))):
    return lax.dot_general(
        left, right, (contract, ((), ())), precision=lax.Precision.HIGHEST, preferred_element_type=F32
    )


def fastdot(left, right, contract):
    return lax.dot_general(left, right, (contract, ((), ())), preferred_element_type=F32)


def split(value):
    high = value.astype(BF16)
    return high, (value - high.astype(F32)).astype(BF16)


def eye(size):
    return (lax.broadcasted_iota(jnp.int32, (size, size), 0) == lax.broadcasted_iota(jnp.int32, (size, size), 1)).astype(F32)


def split3(value):
    high = value.astype(BF16)
    rest = value - high.astype(F32)
    middle = rest.astype(BF16)
    return high, middle, (rest - middle.astype(F32)).astype(BF16)


def tree_sum(terms):
    while len(terms) > 1:
        terms = [sum(terms[i : i + 2]) for i in range(0, len(terms), 2)]
    return terms[0]


def small_step(squared, factor, unit):
    size = unit.shape[0]
    columns = [jnp.broadcast_to(squared[:, k : k + 1], unit.shape) for k in range(size)]
    turn = 1.5 * unit - 0.5 * squared
    turn_columns = [1.5 * unit[:, k : k + 1] - 0.5 * columns[k] for k in range(size)]
    turn_squared = tree_sum([turn_columns[k] * turn[k : k + 1] for k in range(size)])
    factor = tree_sum([turn_columns[k] * factor[k : k + 1] for k in range(size)])
    return tree_sum([columns[k] * turn_squared[k : k + 1] for k in range(size)]), factor


def step(squared, factor, unit):
    if unit.shape[0] <= 16:
        return small_step(squared, factor, unit)
    turn = 1.5 * unit - 0.5 * squared
    if unit.shape[0] % 128:
        return dot(dot(squared, turn), turn), dot(factor, turn)
    high, low = split(squared)
    stacked = jnp.concatenate([high, low, high], axis=0)

    def by_squared(left):
        left_high, left_low = split(left)
        return fastdot(jnp.concatenate([left_high, left_high, left_low], axis=1), stacked, ((1,), (0,)))

    rank = unit.shape[0]
    both = by_squared(jnp.concatenate([squared, factor], axis=0))
    turn = 2.25 * unit - 1.5 * squared + 0.25 * both[:rank]
    return by_squared(turn), 1.5 * factor - 0.5 * both[rank:]


def orth_factor(gram):
    unit = eye(gram.shape[0])
    total = jnp.sum(gram * unit) + TINY
    squared = gram * (1.0 / total)
    factor = unit * lax.rsqrt(total)
    for step_index in range(STEPS):
        squared, factor = step(squared, factor, unit)
    return factor


def halves_of(value):
    high, low = split(value)
    return jnp.concatenate([high, low], axis=1)


def packed_shape(groups_n, cuts, rank, width):
    return (rank, width) if cuts == 1 else (groups_n, cuts, rank // groups_n, width // cuts)


def store(ref, value, add=False):
    if len(ref.shape) == 2:
        ref[...] = ref[...] + value if add else value
        return
    groups_n, cuts, per, piece = ref.shape
    for k in range(cuts):
        part = value[:, k * piece : (k + 1) * piece].reshape(groups_n, per, piece)
        ref[:, k] = ref[:, k] + part if add else part


def load(ref):
    if len(ref.shape) == 2:
        return ref[...]
    groups_n, cuts, per, piece = ref.shape
    return jnp.concatenate([ref[:, k].reshape(groups_n * per, piece) for k in range(cuts)], axis=1)


def project_block(image_high, image_low, factor_both):
    rank = factor_both.shape[1] // 2
    wide = fastdot(factor_both, image_high, ((0,), (0,)))
    return wide[:rank] + wide[rank:] + fastdot(factor_both[:, :rank], image_low, ((0,), (0,)))


def columns_of(part, width):
    return pl.ds(pl.multiple_of(lax.rem(lax.axis_index("rep") + part, lax.axis_size("rep")) * width, width), width)


def first_kernel(image_ref, factor_ref, out_ref, high_ref, low_ref, held_ref, both_ref, fetched_ref, sems, factor_sem):
    blocks = sems.shape[0]
    rows, width = high_ref.shape
    block = rows // blocks
    copies = []
    factor_copy = pltpu.make_async_copy(factor_ref, fetched_ref, factor_sem)
    factor_copy.start()
    for i in range(blocks):
        take = pl.ds(i * block, block)
        copies.append(pltpu.make_async_copy(image_ref.at[take], held_ref.at[take], sems.at[i]))
        copies[-1].start()
    factor_copy.wait()
    both_ref[...] = halves_of(fetched_ref[...])
    columns = columns_of(1, width)
    for i in range(blocks):
        copies[i].wait()
        take = pl.ds(i * block, block)
        high, low = split(held_ref[take, columns])
        high_ref[take] = high
        low_ref[take] = low
        value = project_block(high, low, both_ref[take])
        store(out_ref, value, add=i > 0)


def project_first(image, row_factor, width, packed, blocks=2):
    rows, rank = row_factor.shape
    return pl.pallas_call(
        first_kernel,
        in_specs=[pl.BlockSpec(memory_space=pl.ANY), pl.BlockSpec(memory_space=pl.ANY)],
        out_shape=(
            jax.ShapeDtypeStruct(packed, F32),
            jax.ShapeDtypeStruct((rows, width), BF16),
            jax.ShapeDtypeStruct((rows, width), BF16),
            jax.ShapeDtypeStruct(image.shape, F32),
            jax.ShapeDtypeStruct((rows, 2 * rank), BF16),
        ),
        scratch_shapes=[
            pltpu.VMEM((rows, rank), F32),
            pltpu.SemaphoreType.DMA((blocks,)),
            pltpu.SemaphoreType.DMA,
        ],
        compiler_params=SMALL,
        name="project_first",
    )(
        pltpu.with_memory_space_constraint(image, pltpu.HBM),
        pltpu.with_memory_space_constraint(row_factor, pltpu.HBM),
    )


def second_kernel(blocks, held_ref, both_ref, out_ref, high_ref, low_ref):
    rows, width = high_ref.shape
    block = rows // blocks
    columns = columns_of(0, width)
    total = None
    for i in range(blocks):
        take = pl.ds(i * block, block)
        high, low = split(held_ref[take, columns])
        high_ref[take] = high
        low_ref[take] = low
        value = project_block(high, low, both_ref[take])
        total = value if total is None else total + value
    store(out_ref, total)


def project_second(held, both, width, packed, blocks=4):
    rows, rank = both.shape[0], both.shape[1] // 2
    return pl.pallas_call(
        functools.partial(second_kernel, blocks),
        out_shape=(
            jax.ShapeDtypeStruct(packed, F32),
            jax.ShapeDtypeStruct((rows, width), BF16),
            jax.ShapeDtypeStruct((rows, width), BF16),
        ),
        cost_estimate=pl.CostEstimate(
            flops=6 * rows * width * rank, bytes_accessed=4 * rows * (width + rank), transcendentals=0
        ),
        compiler_params=SMALL,
        name="project_second",
    )(held, both)


def product_kernel(blocks, high_ref, low_ref, weight_ref, *refs):
    out_ref = refs[-1]
    weight_high, weight_low = split(load(weight_ref))
    rank = weight_high.shape[0]
    both = jnp.concatenate([weight_high, weight_low], axis=0)
    block = out_ref.shape[0] // blocks
    for i in range(blocks):
        take = pl.ds(i * block, block)
        wide = fastdot(high_ref[take], both, ((1,), (1,)))
        value = wide[:, :rank] + wide[:, rank:] + fastdot(low_ref[take], weight_high, ((1,), (1,)))
        if len(refs) > 1:
            value = value + refs[0][take]
        out_ref[take] = value


def multiply(high, low, weight, start=None, blocks=4):
    rows, width = high.shape
    rank = weight.size // width
    more = () if start is None else (start,)
    return pl.pallas_call(
        functools.partial(product_kernel, blocks),
        out_shape=jax.ShapeDtypeStruct((rows, rank), F32),
        cost_estimate=pl.CostEstimate(
            flops=6 * rows * width * rank, bytes_accessed=4 * rows * (width + rank), transcendentals=0
        ),
        compiler_params=SMALL,
        name="multiply",
    )(high, low, weight, *more)


def cells(rows, count, row_of, cell_of):
    row = row_of(lax.broadcasted_iota(jnp.int32, (rows, count), 0))
    return (row == cell_of(lax.broadcasted_iota(jnp.int32, (rows, count), 1))).astype(F32)


def spread(groups_n, rank):
    per = rank // groups_n
    return cells(rank, groups_n, lambda row: row // per, lambda cell: cell)


def same_slot(groups_n, rank):
    per = rank // groups_n
    return cells(rank, rank, lambda row: row % per, lambda cell: cell % per) > 0.5


def gram_kernel(groups_n, owned_ref, out_ref):
    high, low = split(load(owned_ref))
    rank = high.shape[0]
    per = rank // groups_n
    wide = fastdot(high, jnp.concatenate([high, low], axis=0), ((1,), (1,)))
    full = wide[:, :rank] + wide[:, rank:] + wide[:, rank:].T
    full = jnp.where(same_slot(groups_n, rank), full, 0.0)
    if len(out_ref.shape) == 2:
        fold = spread(groups_n, rank)
        out_ref[...] = dot(dot(fold, full, ((0,), (0,))), fold)
    else:
        count = out_ref.shape[2]
        columns = cells(rank, count, lambda row: row // per, lambda cell: cell % groups_n).astype(BF16)
        folded = fastdot(
            jnp.concatenate(split3(full), axis=1), jnp.concatenate([columns, columns, columns], axis=0), ((1,), (0,))
        )
        rows = cells(rank, count, lambda row: row // per, lambda cell: cell // groups_n)
        flat = jnp.sum(rows * folded, axis=0, keepdims=True)
        out_ref[...] = jnp.broadcast_to(flat[None], out_ref.shape)


def small_gram(owned, groups_n, shape):
    return pl.pallas_call(
        functools.partial(gram_kernel, groups_n),
        out_shape=jax.ShapeDtypeStruct(shape, F32),
        compiler_params=SMALL,
        name="small_gram",
    )(owned)


def mix_kernel(groups_n, gram_ref, time_ref, owned_ref, out_ref, time_out_ref):
    owned_high, owned_low = split(load(owned_ref))
    rank = owned_high.shape[0]
    per = rank // groups_n
    if len(gram_ref.shape) == 2:
        fold = spread(groups_n, rank)
        start = dot(fold, dot(gram_ref[...], time_ref[...], ((1,), (1,))))
        turned = dot(dot(time_ref[...], gram_ref[...], ((1,), (1,))), fold, ((1,), (1,)))
    else:
        count = gram_ref.shape[2]
        flat = jnp.sum(gram_ref[...], axis=0)
        rows = cells(rank, count, lambda row: row // per, lambda cell: cell // groups_n) * flat
        columns = dot(time_ref[...], cells(groups_n, count, lambda row: row, lambda cell: cell % groups_n))
        start = dot(rows, columns, ((1,), (1,)))
        turned = dot(columns, rows, ((1,), (1,)))
    basis = dot(start, orth_factor(dot(turned, start) * (1.0 / per)))
    mixer = jnp.where(same_slot(groups_n, rank), dot(basis, basis, ((1,), (1,))), 0.0)
    mixer_high, mixer_low = split(mixer)
    mixed = fastdot(
        jnp.concatenate([mixer_high, mixer_low, mixer_high], axis=1),
        jnp.concatenate([owned_high, owned_high, owned_low], axis=0),
        ((1,), (0,)),
    )
    store(out_ref, mixed)
    one_of_each = cells(groups_n, rank, lambda row: row * per, lambda cell: cell)
    time_out_ref[...] = dot(one_of_each, basis) * math.sqrt(groups_n)


def mix(gram, time_factor, owned, groups_n):
    return pl.pallas_call(
        functools.partial(mix_kernel, groups_n),
        out_shape=(jax.ShapeDtypeStruct(owned.shape, F32), jax.ShapeDtypeStruct(time_factor.shape, F32)),
        compiler_params=SMALL,
        name="mix",
    )(gram, time_factor.T, owned)


def finish_kernel(scale, blocks, block_ref, mine_ref, other_ref, out_ref, made_ref, sems):
    rows = block_ref.shape[0] // blocks
    high, low = split(block_ref[...])
    left = jnp.concatenate([high, low, high], axis=1)
    factor_high, factor_low = split(orth_factor(mine_ref[...] + other_ref[...]) * scale)
    right = jnp.concatenate([factor_high, factor_high, factor_low], axis=0)
    copies = []
    for i in range(blocks):
        take = pl.ds(i * rows, rows)
        made_ref[take] = fastdot(left[i * rows : (i + 1) * rows], right, ((1,), (0,)))
        copies.append(pltpu.make_async_copy(made_ref.at[take], out_ref.at[take], sems.at[i]))
        copies[-1].start()
    for copy in copies:
        copy.wait()


def finish(block, mine, other, scale, blocks=4):
    return pl.pallas_call(
        functools.partial(finish_kernel, scale, blocks),
        out_shape=jax.ShapeDtypeStruct(block.shape, F32),
        out_specs=pl.BlockSpec(memory_space=pl.ANY),
        scratch_shapes=[pltpu.VMEM(block.shape, F32), pltpu.SemaphoreType.DMA((blocks,))],
        compiler_params=SMALL,
        name="finish",
    )(block, mine, other)


def row_gram_kernel(block_ref, out_ref):
    high, low = split(block_ref[...])
    rank = high.shape[1]
    wide = fastdot(high, jnp.concatenate([high, low], axis=1), ((0,), (0,)))
    out_ref[...] = wide[:, :rank] + wide[:, rank:] + wide[:, rank:].T


def row_gram(block):
    rank = block.shape[1]
    return pl.pallas_call(row_gram_kernel, out_shape=jax.ShapeDtypeStruct((rank, rank), F32), compiler_params=SMALL, name="row_gram")(block)


def make_on_device(groups_n, reps):
    half_n = groups_n // 2
    halves = [[h * half_n + i for i in range(half_n)] for h in range(2)]
    across = [(i, (i + half_n) % groups_n) for i in range(groups_n)]
    swap = [(0, 1), (1, 0)]

    def all_to_all(value, parts, groups=None):
        shape = value.shape
        value = value.reshape((parts, shape[0] // parts) + shape[1:])
        value = lax.all_to_all(value, "grp", split_axis=0, concat_axis=0, tiled=True, axis_index_groups=groups)
        return value.reshape(shape)

    def to_owners(value):
        if len(value.shape) == 2:
            return all_to_all(value, groups_n)
        flat = value.reshape((groups_n * reps,) + value.shape[2:])
        return lax.all_to_all(flat, ("grp", "rep"), split_axis=0, concat_axis=0, tiled=True).reshape(value.shape)

    def on_device(snapshots, row_factor, time_factor):
        rows, cols = snapshots.shape[1:]
        rank = row_factor.shape[1]
        width = cols // reps
        fits = rank % (8 * groups_n) == 0 and width % (128 * reps) == 0
        packed = packed_shape(groups_n, reps if fits else 1, rank, width)
        send, far_high, far_low, held, both = project_first(snapshots[0], row_factor, width, packed)
        received = lax.ppermute(send, "rep", swap)
        summed, near_high, near_low = project_second(held, both, width, packed)
        summed = summed + received
        owned = to_owners(summed)
        devices = groups_n * reps
        if devices * groups_n * groups_n <= 1 << 20:
            grams = lax.all_to_all(
                small_gram(owned, groups_n, (devices, 1, groups_n * groups_n)),
                ("grp", "rep"),
                split_axis=0,
                concat_axis=0,
                tiled=True,
            )
        else:
            grams = lax.psum(small_gram(owned, groups_n, (groups_n, groups_n)), ("grp", "rep"))
        weights, new_time = mix(grams, time_factor, owned, groups_n)
        weight = to_owners(weights)
        other_weight = lax.ppermute(weight, "rep", swap)
        product = multiply(far_high, far_low, other_weight, multiply(near_high, near_low, weight))
        parts = all_to_all(product, half_n, halves)
        chunk = jnp.sum(parts.reshape(half_n, rows // half_n, rank), axis=0)
        chunk = chunk + lax.ppermute(chunk, "grp", across)
        block = all_to_all(jnp.tile(chunk, (half_n, 1)), half_n, halves)
        gram = row_gram(block)
        new_rows = finish(block, gram, lax.ppermute(gram, "rep", swap), math.sqrt(rows * reps))
        return (new_rows, new_time)

    return on_device


def solution(mesh):
    return jax.shard_map(
        make_on_device(mesh.shape["grp"], mesh.shape["rep"]),
        mesh=mesh,
        in_specs=(P("grp", "rep", None), P("rep", None), P()),
        out_specs=(P("rep", None), P()),
        check_vma=False,
    )
```

```python
import functools
import math

import jax
import jax.numpy as jnp
from jax import lax
from jax.experimental import pallas as pl
from jax.experimental.pallas import tpu as pltpu
from jax.sharding import PartitionSpec as P

STEPS = 8
SMALL = pltpu.CompilerParams(vmem_limit_bytes=16 << 20)
F32 = jnp.float32
BF16 = jnp.bfloat16
TINY = 1e-06


def dot(left, right, contract=((1,), (0,))):
    return lax.dot_general(
        left, right, (contract, ((), ())), precision=lax.Precision.HIGHEST, preferred_element_type=F32
    )


def fastdot(left, right, contract):
    return lax.dot_general(left, right, (contract, ((), ())), preferred_element_type=F32)


def split(value):
    high = value.astype(BF16)
    return high, (value - high.astype(F32)).astype(BF16)


def eye(size):
    return (lax.broadcasted_iota(jnp.int32, (size, size), 0) == lax.broadcasted_iota(jnp.int32, (size, size), 1)).astype(F32)


def split3(value):
    high = value.astype(BF16)
    rest = value - high.astype(F32)
    middle = rest.astype(BF16)
    return high, middle, (rest - middle.astype(F32)).astype(BF16)


def halves_of(value):
    high, low = split(value)
    return jnp.concatenate([high, low], axis=1)


def stack(right):
    both = halves_of(right)
    return jnp.concatenate([both, both], axis=0)


def by_stacked(left_halves, stacked):
    wide = fastdot(left_halves, stacked, ((1,), (0,)))
    size = stacked.shape[1] // 2
    return wide[:, :size] + wide[:, size:]


def tree_sum(terms):
    while len(terms) > 1:
        terms = [sum(terms[i : i + 2]) for i in range(0, len(terms), 2)]
    return terms[0]


def small_step(squared, factor, unit):
    size = unit.shape[0]
    columns = [jnp.broadcast_to(squared[:, k : k + 1], unit.shape) for k in range(size)]
    turn = 1.5 * unit - 0.5 * squared
    turn_columns = [1.5 * unit[:, k : k + 1] - 0.5 * columns[k] for k in range(size)]
    turn_squared = tree_sum([turn_columns[k] * turn[k : k + 1] for k in range(size)])
    factor = tree_sum([turn_columns[k] * factor[k : k + 1] for k in range(size)])
    return tree_sum([columns[k] * turn_squared[k : k + 1] for k in range(size)]), factor


def step(squared, factor, unit):
    if unit.shape[0] <= 16:
        return small_step(squared, factor, unit)
    turn = 1.5 * unit - 0.5 * squared
    if unit.shape[0] % 128:
        return dot(dot(squared, turn), turn), dot(factor, turn)
    rank = unit.shape[0]
    stacked = stack(squared)
    both = by_stacked(halves_of(jnp.concatenate([squared, factor], axis=0)), stacked)
    turn = 2.25 * unit - 1.5 * squared + 0.25 * both[:rank]
    return by_stacked(halves_of(turn), stacked), 1.5 * factor - 0.5 * both[rank:]


def orth_factor(gram):
    unit = eye(gram.shape[0])
    total = jnp.sum(gram * unit) + TINY
    squared = gram * (1.0 / total)
    factor = unit * lax.rsqrt(total)
    for step_index in range(STEPS):
        squared, factor = step(squared, factor, unit)
    return factor


def packed_shape(groups_n, cuts, rank, width):
    return (rank, width) if cuts == 1 else (groups_n, cuts, rank // groups_n, width // cuts)


def store(ref, value, add=False):
    if len(ref.shape) == 2:
        ref[...] = ref[...] + value if add else value
        return
    groups_n, cuts, per, piece = ref.shape
    for k in range(cuts):
        part = value[:, k * piece : (k + 1) * piece].reshape(groups_n, per, piece)
        ref[:, k] = ref[:, k] + part if add else part


def load(ref):
    if len(ref.shape) == 2:
        return ref[...]
    groups_n, cuts, per, piece = ref.shape
    return jnp.concatenate([ref[:, k].reshape(groups_n * per, piece) for k in range(cuts)], axis=1)


def project_block(image_high, image_low, factor_both):
    rank = factor_both.shape[1] // 2
    wide = fastdot(factor_both, image_high, ((0,), (0,)))
    return wide[:rank] + wide[rank:] + fastdot(factor_both[:, :rank], image_low, ((0,), (0,)))


def columns_of(part, width):
    return pl.ds(pl.multiple_of(lax.rem(lax.axis_index("rep") + part, lax.axis_size("rep")) * width, width), width)


def first_kernel(image_ref, factor_ref, out_ref, high_ref, low_ref, held_ref, both_ref, fetched_ref, sems, factor_sem):
    blocks = sems.shape[0]
    rows, width = high_ref.shape
    block = rows // blocks
    copies = []
    factor_copy = pltpu.make_async_copy(factor_ref, fetched_ref, factor_sem)
    factor_copy.start()
    for i in range(blocks):
        take = pl.ds(i * block, block)
        copies.append(pltpu.make_async_copy(image_ref.at[take], held_ref.at[take], sems.at[i]))
        copies[-1].start()
    factor_copy.wait()
    both_ref[...] = halves_of(fetched_ref[...])
    columns = columns_of(1, width)
    for i in range(blocks):
        copies[i].wait()
        take = pl.ds(i * block, block)
        high, low = split(held_ref[take, columns])
        high_ref[take] = high
        low_ref[take] = low
        value = project_block(high, low, both_ref[take])
        store(out_ref, value, add=i > 0)


def project_first(image, row_factor, width, packed, blocks=2):
    rows, rank = row_factor.shape
    return pl.pallas_call(
        first_kernel,
        in_specs=[pl.BlockSpec(memory_space=pl.ANY), pl.BlockSpec(memory_space=pl.ANY)],
        out_shape=(
            jax.ShapeDtypeStruct(packed, F32),
            jax.ShapeDtypeStruct((rows, width), BF16),
            jax.ShapeDtypeStruct((rows, width), BF16),
            jax.ShapeDtypeStruct(image.shape, F32),
            jax.ShapeDtypeStruct((rows, 2 * rank), BF16),
        ),
        scratch_shapes=[
            pltpu.VMEM((rows, rank), F32),
            pltpu.SemaphoreType.DMA((blocks,)),
            pltpu.SemaphoreType.DMA,
        ],
        compiler_params=SMALL,
        name="project_first",
    )(
        pltpu.with_memory_space_constraint(image, pltpu.HBM),
        pltpu.with_memory_space_constraint(row_factor, pltpu.HBM),
    )


def second_kernel(blocks, held_ref, both_ref, out_ref, high_ref, low_ref):
    rows, width = high_ref.shape
    block = rows // blocks
    columns = columns_of(0, width)
    total = None
    for i in range(blocks):
        take = pl.ds(i * block, block)
        high, low = split(held_ref[take, columns])
        high_ref[take] = high
        low_ref[take] = low
        value = project_block(high, low, both_ref[take])
        total = value if total is None else total + value
    store(out_ref, total)


def project_second(held, both, width, packed, blocks=4):
    rows, rank = both.shape[0], both.shape[1] // 2
    return pl.pallas_call(
        functools.partial(second_kernel, blocks),
        out_shape=(
            jax.ShapeDtypeStruct(packed, F32),
            jax.ShapeDtypeStruct((rows, width), BF16),
            jax.ShapeDtypeStruct((rows, width), BF16),
        ),
        cost_estimate=pl.CostEstimate(
            flops=6 * rows * width * rank, bytes_accessed=4 * rows * (width + rank), transcendentals=0
        ),
        compiler_params=SMALL,
        name="project_second",
    )(held, both)


def product_kernel(blocks, high_ref, low_ref, weight_ref, *refs):
    out_ref = refs[-1]
    weight_high, weight_low = split(load(weight_ref))
    rank = weight_high.shape[0]
    both = jnp.concatenate([weight_high, weight_low], axis=0)
    block = out_ref.shape[0] // blocks
    for i in range(blocks):
        take = pl.ds(i * block, block)
        wide = fastdot(high_ref[take], both, ((1,), (1,)))
        value = wide[:, :rank] + wide[:, rank:] + fastdot(low_ref[take], weight_high, ((1,), (1,)))
        if len(refs) > 1:
            value = value + refs[0][take]
        out_ref[take] = value


def multiply(high, low, weight, start=None, blocks=4):
    rows, width = high.shape
    rank = weight.size // width
    more = () if start is None else (start,)
    return pl.pallas_call(
        functools.partial(product_kernel, blocks),
        out_shape=jax.ShapeDtypeStruct((rows, rank), F32),
        cost_estimate=pl.CostEstimate(
            flops=6 * rows * width * rank, bytes_accessed=4 * rows * (width + rank), transcendentals=0
        ),
        compiler_params=SMALL,
        name="multiply",
    )(high, low, weight, *more)


def cells(rows, count, row_of, cell_of):
    row = row_of(lax.broadcasted_iota(jnp.int32, (rows, count), 0))
    return (row == cell_of(lax.broadcasted_iota(jnp.int32, (rows, count), 1))).astype(F32)


def spread(groups_n, rank):
    per = rank // groups_n
    return cells(rank, groups_n, lambda row: row // per, lambda cell: cell)


def same_slot(groups_n, rank):
    per = rank // groups_n
    return cells(rank, rank, lambda row: row % per, lambda cell: cell % per) > 0.5


def gram_kernel(groups_n, owned_ref, out_ref):
    high, low = split(load(owned_ref))
    rank = high.shape[0]
    per = rank // groups_n
    wide = fastdot(high, jnp.concatenate([high, low], axis=0), ((1,), (1,)))
    full = wide[:, :rank] + wide[:, rank:] + wide[:, rank:].T
    full = jnp.where(same_slot(groups_n, rank), full, 0.0)
    if len(out_ref.shape) == 2:
        fold = spread(groups_n, rank)
        out_ref[...] = dot(dot(fold, full, ((0,), (0,))), fold)
    else:
        count = out_ref.shape[2]
        columns = cells(rank, count, lambda row: row // per, lambda cell: cell % groups_n).astype(BF16)
        folded = fastdot(
            jnp.concatenate(split3(full), axis=1), jnp.concatenate([columns, columns, columns], axis=0), ((1,), (0,))
        )
        rows = cells(rank, count, lambda row: row // per, lambda cell: cell // groups_n)
        flat = jnp.sum(rows * folded, axis=0, keepdims=True)
        out_ref[...] = jnp.broadcast_to(flat[None], out_ref.shape)


def small_gram(owned, groups_n, shape):
    return pl.pallas_call(
        functools.partial(gram_kernel, groups_n),
        out_shape=jax.ShapeDtypeStruct(shape, F32),
        compiler_params=SMALL,
        name="small_gram",
    )(owned)


def mix_kernel(groups_n, gram_ref, time_ref, owned_ref, out_ref, time_out_ref):
    owned_high, owned_low = split(load(owned_ref))
    rank = owned_high.shape[0]
    per = rank // groups_n
    if len(gram_ref.shape) == 2:
        fold = spread(groups_n, rank)
        start = dot(fold, dot(gram_ref[...], time_ref[...], ((1,), (1,))))
        turned = dot(dot(time_ref[...], gram_ref[...], ((1,), (1,))), fold, ((1,), (1,)))
    else:
        count = gram_ref.shape[2]
        flat = jnp.sum(gram_ref[...], axis=0)
        rows = cells(rank, count, lambda row: row // per, lambda cell: cell // groups_n) * flat
        columns = dot(time_ref[...], cells(groups_n, count, lambda row: row, lambda cell: cell % groups_n))
        start = dot(rows, columns, ((1,), (1,)))
        turned = dot(columns, rows, ((1,), (1,)))
    basis = dot(start, orth_factor(dot(turned, start) * (1.0 / per)))
    mixer = jnp.where(same_slot(groups_n, rank), dot(basis, basis, ((1,), (1,))), 0.0)
    mixer_high, mixer_low = split(mixer)
    mixed = fastdot(
        jnp.concatenate([mixer_high, mixer_low, mixer_high], axis=1),
        jnp.concatenate([owned_high, owned_high, owned_low], axis=0),
        ((1,), (0,)),
    )
    store(out_ref, mixed)
    one_of_each = cells(groups_n, rank, lambda row: row * per, lambda cell: cell)
    time_out_ref[...] = dot(one_of_each, basis) * math.sqrt(groups_n)


def mix(gram, time_factor, owned, groups_n):
    return pl.pallas_call(
        functools.partial(mix_kernel, groups_n),
        out_shape=(jax.ShapeDtypeStruct(owned.shape, F32), jax.ShapeDtypeStruct(time_factor.shape, F32)),
        compiler_params=SMALL,
        name="mix",
    )(gram, time_factor.T, owned)


def finish_kernel(scale, blocks, block_ref, mine_ref, other_ref, out_ref, made_ref, sems):
    rows = block_ref.shape[0] // blocks
    left = halves_of(block_ref[...])
    right = stack(orth_factor(mine_ref[...] + other_ref[...]) * scale)
    copies = []
    for i in range(blocks):
        take = pl.ds(i * rows, rows)
        made_ref[take] = by_stacked(left[i * rows : (i + 1) * rows], right)
        copies.append(pltpu.make_async_copy(made_ref.at[take], out_ref.at[take], sems.at[i]))
        copies[-1].start()
    for copy in copies:
        copy.wait()


def finish(block, mine, other, scale, blocks=4):
    return pl.pallas_call(
        functools.partial(finish_kernel, scale, blocks),
        out_shape=jax.ShapeDtypeStruct(block.shape, F32),
        out_specs=pl.BlockSpec(memory_space=pl.ANY),
        scratch_shapes=[pltpu.VMEM(block.shape, F32), pltpu.SemaphoreType.DMA((blocks,))],
        compiler_params=SMALL,
        name="finish",
    )(block, mine, other)


def row_gram_kernel(block_ref, out_ref):
    high, low = split(block_ref[...])
    rank = high.shape[1]
    wide = fastdot(high, jnp.concatenate([high, low], axis=1), ((0,), (0,)))
    out_ref[...] = wide[:, :rank] + wide[:, rank:] + wide[:, rank:].T


def row_gram(block):
    rank = block.shape[1]
    return pl.pallas_call(row_gram_kernel, out_shape=jax.ShapeDtypeStruct((rank, rank), F32), compiler_params=SMALL, name="row_gram")(block)


def make_on_device(groups_n, reps):
    half_n = groups_n // 2
    halves = [[h * half_n + i for i in range(half_n)] for h in range(2)]
    across = [(i, (i + half_n) % groups_n) for i in range(groups_n)]
    swap = [(0, 1), (1, 0)]

    def all_to_all(value, parts, groups=None):
        shape = value.shape
        value = value.reshape((parts, shape[0] // parts) + shape[1:])
        value = lax.all_to_all(value, "grp", split_axis=0, concat_axis=0, tiled=True, axis_index_groups=groups)
        return value.reshape(shape)

    def to_owners(value):
        if len(value.shape) == 2:
            return all_to_all(value, groups_n)
        flat = value.reshape((groups_n * reps,) + value.shape[2:])
        return lax.all_to_all(flat, ("grp", "rep"), split_axis=0, concat_axis=0, tiled=True).reshape(value.shape)

    def on_device(snapshots, row_factor, time_factor):
        rows, cols = snapshots.shape[1:]
        rank = row_factor.shape[1]
        width = cols // reps
        fits = rank % (8 * groups_n) == 0 and width % (128 * reps) == 0
        packed = packed_shape(groups_n, reps if fits else 1, rank, width)
        send, far_high, far_low, held, both = project_first(snapshots[0], row_factor, width, packed)
        received = lax.ppermute(send, "rep", swap)
        summed, near_high, near_low = project_second(held, both, width, packed)
        summed = summed + received
        owned = to_owners(summed)
        devices = groups_n * reps
        if devices * groups_n * groups_n <= 1 << 20:
            grams = lax.all_to_all(
                small_gram(owned, groups_n, (devices, 1, groups_n * groups_n)),
                ("grp", "rep"),
                split_axis=0,
                concat_axis=0,
                tiled=True,
            )
        else:
            grams = lax.psum(small_gram(owned, groups_n, (groups_n, groups_n)), ("grp", "rep"))
        weights, new_time = mix(grams, time_factor, owned, groups_n)
        weight = to_owners(weights)
        other_weight = lax.ppermute(weight, "rep", swap)
        product = multiply(far_high, far_low, other_weight, multiply(near_high, near_low, weight))
        parts = all_to_all(product, half_n, halves)
        chunk = jnp.sum(parts.reshape(half_n, rows // half_n, rank), axis=0)
        chunk = chunk + lax.ppermute(chunk, "grp", across)
        block = all_to_all(jnp.tile(chunk, (half_n, 1)), half_n, halves)
        gram = row_gram(block)
        new_rows = finish(block, gram, lax.ppermute(gram, "rep", swap), math.sqrt(rows * reps))
        return (new_rows, new_time)

    return on_device


def solution(mesh):
    return jax.shard_map(
        make_on_device(mesh.shape["grp"], mesh.shape["rep"]),
        mesh=mesh,
        in_specs=(P("grp", "rep", None), P("rep", None), P()),
        out_specs=(P("rep", None), P()),
        check_vma=False,
    )
```

```python
import functools
import math

import jax
import jax.numpy as jnp
from jax import lax
from jax.experimental import pallas as pl
from jax.experimental.pallas import tpu as pltpu
from jax.sharding import PartitionSpec as P

STEPS = 8
SMALL = pltpu.CompilerParams(vmem_limit_bytes=16 << 20)
F32 = jnp.float32
BF16 = jnp.bfloat16
TINY = 1e-06


def dot(left, right, contract=((1,), (0,))):
    return lax.dot_general(
        left, right, (contract, ((), ())), precision=lax.Precision.HIGHEST, preferred_element_type=F32
    )


def fastdot(left, right, contract):
    return lax.dot_general(left, right, (contract, ((), ())), preferred_element_type=F32)


def split(value):
    high = value.astype(BF16)
    return high, (value - high.astype(F32)).astype(BF16)


def eye(size):
    return (lax.broadcasted_iota(jnp.int32, (size, size), 0) == lax.broadcasted_iota(jnp.int32, (size, size), 1)).astype(F32)


def split3(value):
    high = value.astype(BF16)
    rest = value - high.astype(F32)
    middle = rest.astype(BF16)
    return high, middle, (rest - middle.astype(F32)).astype(BF16)


def halves_of(value):
    high, low = split(value)
    return jnp.concatenate([high, low], axis=1)


def stack(right):
    both = halves_of(right)
    return jnp.concatenate([both, both], axis=0)


def by_stacked(left_halves, stacked):
    wide = fastdot(left_halves, stacked, ((1,), (0,)))
    size = stacked.shape[1] // 2
    return wide[:, :size] + wide[:, size:]


def tree_sum(terms):
    while len(terms) > 1:
        terms = [sum(terms[i : i + 2]) for i in range(0, len(terms), 2)]
    return terms[0]


def small_step(squared, factor, unit):
    size = unit.shape[0]
    columns = [jnp.broadcast_to(squared[:, k : k + 1], unit.shape) for k in range(size)]
    turn = 1.5 * unit - 0.5 * squared
    turn_columns = [1.5 * unit[:, k : k + 1] - 0.5 * columns[k] for k in range(size)]
    turn_squared = tree_sum([turn_columns[k] * turn[k : k + 1] for k in range(size)])
    factor = tree_sum([turn_columns[k] * factor[k : k + 1] for k in range(size)])
    return tree_sum([columns[k] * turn_squared[k : k + 1] for k in range(size)]), factor


def step(squared, factor, unit):
    if unit.shape[0] <= 16:
        return small_step(squared, factor, unit)
    turn = 1.5 * unit - 0.5 * squared
    if unit.shape[0] % 128:
        return dot(dot(squared, turn), turn), dot(factor, turn)
    rank = unit.shape[0]
    stacked = stack(squared)
    both = by_stacked(halves_of(jnp.concatenate([squared, factor], axis=0)), stacked)
    turn = 2.25 * unit - 1.5 * squared + 0.25 * both[:rank]
    return by_stacked(halves_of(turn), stacked), 1.5 * factor - 0.5 * both[rank:]


def orth_factor(gram):
    unit = eye(gram.shape[0])
    total = jnp.sum(gram * unit) + TINY
    squared = gram * (1.0 / total)
    factor = unit * lax.rsqrt(total)
    for step_index in range(STEPS):
        squared, factor = step(squared, factor, unit)
    return factor


def packed_shape(groups_n, cuts, rank, width):
    return (rank, width) if cuts == 1 else (groups_n, cuts, rank // groups_n, width // cuts)


def store(ref, value, add=False):
    if len(ref.shape) == 2:
        ref[...] = ref[...] + value if add else value
        return
    groups_n, cuts, per, piece = ref.shape
    for k in range(cuts):
        part = value[:, k * piece : (k + 1) * piece].reshape(groups_n, per, piece)
        ref[:, k] = ref[:, k] + part if add else part


def load(ref):
    if len(ref.shape) == 2:
        return ref[...]
    groups_n, cuts, per, piece = ref.shape
    return jnp.concatenate([ref[:, k].reshape(groups_n * per, piece) for k in range(cuts)], axis=1)


def project_block(image_high, image_low, factor_both):
    rank = factor_both.shape[1] // 2
    wide = fastdot(factor_both, image_high, ((0,), (0,)))
    return wide[:rank] + wide[rank:] + fastdot(factor_both[:, :rank], image_low, ((0,), (0,)))


def columns_of(part, width):
    return pl.ds(pl.multiple_of(lax.rem(lax.axis_index("rep") + part, lax.axis_size("rep")) * width, width), width)


def first_kernel(image_ref, factor_ref, out_ref, high_ref, low_ref, held_ref, both_ref, fetched_ref, sems, factor_sem):
    blocks = sems.shape[0]
    rows, width = high_ref.shape
    block = rows // blocks
    copies = []
    factor_copy = pltpu.make_async_copy(factor_ref, fetched_ref, factor_sem)
    factor_copy.start()
    for i in range(blocks):
        take = pl.ds(i * block, block)
        copies.append(pltpu.make_async_copy(image_ref.at[take], held_ref.at[take], sems.at[i]))
        copies[-1].start()
    factor_copy.wait()
    both_ref[...] = halves_of(fetched_ref[...])
    columns = columns_of(1, width)
    for i in range(blocks):
        copies[i].wait()
        take = pl.ds(i * block, block)
        high, low = split(held_ref[take, columns])
        high_ref[take] = high
        low_ref[take] = low
        value = project_block(high, low, both_ref[take])
        store(out_ref, value, add=i > 0)


def project_first(image, row_factor, width, packed, blocks=2):
    rows, rank = row_factor.shape
    return pl.pallas_call(
        first_kernel,
        in_specs=[pl.BlockSpec(memory_space=pl.ANY), pl.BlockSpec(memory_space=pl.ANY)],
        out_shape=(
            jax.ShapeDtypeStruct(packed, F32),
            jax.ShapeDtypeStruct((rows, width), BF16),
            jax.ShapeDtypeStruct((rows, width), BF16),
            jax.ShapeDtypeStruct(image.shape, F32),
            jax.ShapeDtypeStruct((rows, 2 * rank), BF16),
        ),
        scratch_shapes=[
            pltpu.VMEM((rows, rank), F32),
            pltpu.SemaphoreType.DMA((blocks,)),
            pltpu.SemaphoreType.DMA,
        ],
        compiler_params=SMALL,
        name="project_first",
    )(
        pltpu.with_memory_space_constraint(image, pltpu.HBM),
        pltpu.with_memory_space_constraint(row_factor, pltpu.HBM),
    )


def second_kernel(blocks, held_ref, both_ref, out_ref, high_ref, low_ref):
    rows, width = high_ref.shape
    block = rows // blocks
    columns = columns_of(0, width)
    total = None
    for i in range(blocks):
        take = pl.ds(i * block, block)
        high, low = split(held_ref[take, columns])
        high_ref[take] = high
        low_ref[take] = low
        value = project_block(high, low, both_ref[take])
        total = value if total is None else total + value
    store(out_ref, total)


def project_second(held, both, width, packed, blocks=4):
    rows, rank = both.shape[0], both.shape[1] // 2
    return pl.pallas_call(
        functools.partial(second_kernel, blocks),
        out_shape=(
            jax.ShapeDtypeStruct(packed, F32),
            jax.ShapeDtypeStruct((rows, width), BF16),
            jax.ShapeDtypeStruct((rows, width), BF16),
        ),
        cost_estimate=pl.CostEstimate(
            flops=6 * rows * width * rank, bytes_accessed=4 * rows * (width + rank), transcendentals=0
        ),
        compiler_params=SMALL,
        name="project_second",
    )(held, both)


def product_kernel(blocks, high_ref, low_ref, weight_ref, *refs):
    out_ref = refs[-1]
    weight_high, weight_low = split(load(weight_ref))
    rank = weight_high.shape[0]
    both = jnp.concatenate([weight_high, weight_low], axis=0)
    block = out_ref.shape[0] // blocks
    for i in range(blocks):
        take = pl.ds(i * block, block)
        wide = fastdot(high_ref[take], both, ((1,), (1,)))
        value = wide[:, :rank] + wide[:, rank:] + fastdot(low_ref[take], weight_high, ((1,), (1,)))
        if len(refs) > 1:
            value = value + refs[0][take]
        out_ref[take] = value


def multiply(high, low, weight, start=None, blocks=4):
    rows, width = high.shape
    rank = weight.size // width
    more = () if start is None else (start,)
    return pl.pallas_call(
        functools.partial(product_kernel, blocks),
        out_shape=jax.ShapeDtypeStruct((rows, rank), F32),
        cost_estimate=pl.CostEstimate(
            flops=6 * rows * width * rank, bytes_accessed=4 * rows * (width + rank), transcendentals=0
        ),
        compiler_params=SMALL,
        name="multiply",
    )(high, low, weight, *more)


def cells(rows, count, row_of, cell_of):
    row = row_of(lax.broadcasted_iota(jnp.int32, (rows, count), 0))
    return (row == cell_of(lax.broadcasted_iota(jnp.int32, (rows, count), 1))).astype(F32)


def spread(groups_n, rank):
    per = rank // groups_n
    return cells(rank, groups_n, lambda row: row // per, lambda cell: cell)


def same_slot(groups_n, rank):
    per = rank // groups_n
    return cells(rank, rank, lambda row: row % per, lambda cell: cell % per) > 0.5


def gram_kernel(groups_n, owned_ref, out_ref):
    high, low = split(load(owned_ref))
    rank = high.shape[0]
    per = rank // groups_n
    wide = fastdot(high, jnp.concatenate([high, low], axis=0), ((1,), (1,)))
    full = wide[:, :rank] + wide[:, rank:] + wide[:, rank:].T
    full = jnp.where(same_slot(groups_n, rank), full, 0.0)
    if len(out_ref.shape) == 2:
        fold = spread(groups_n, rank)
        out_ref[...] = dot(dot(fold, full, ((0,), (0,))), fold)
    else:
        count = out_ref.shape[2]
        columns = cells(rank, count, lambda row: row // per, lambda cell: cell % groups_n).astype(BF16)
        folded = fastdot(
            jnp.concatenate(split3(full), axis=1), jnp.concatenate([columns, columns, columns], axis=0), ((1,), (0,))
        )
        rows = cells(rank, count, lambda row: row // per, lambda cell: cell // groups_n)
        flat = jnp.sum(rows * folded, axis=0, keepdims=True)
        out_ref[...] = jnp.broadcast_to(flat[None], out_ref.shape)


def small_gram(owned, groups_n, shape):
    return pl.pallas_call(
        functools.partial(gram_kernel, groups_n),
        out_shape=jax.ShapeDtypeStruct(shape, F32),
        compiler_params=SMALL,
        name="small_gram",
    )(owned)


def mix_kernel(groups_n, gram_ref, time_ref, owned_ref, out_ref, time_out_ref):
    owned_high, owned_low = split(load(owned_ref))
    rank = owned_high.shape[0]
    per = rank // groups_n
    if len(gram_ref.shape) == 2:
        fold = spread(groups_n, rank)
        start = dot(fold, dot(gram_ref[...], time_ref[...], ((1,), (1,))))
        turned = dot(dot(time_ref[...], gram_ref[...], ((1,), (1,))), fold, ((1,), (1,)))
    else:
        count = gram_ref.shape[2]
        flat = jnp.sum(gram_ref[...], axis=0)
        rows = cells(rank, count, lambda row: row // per, lambda cell: cell // groups_n) * flat
        columns = dot(time_ref[...], cells(groups_n, count, lambda row: row, lambda cell: cell % groups_n))
        start = dot(rows, columns, ((1,), (1,)))
        turned = dot(columns, rows, ((1,), (1,)))
    basis = dot(start, orth_factor(dot(turned, start) * (1.0 / per)))
    mixer = jnp.where(same_slot(groups_n, rank), dot(basis, basis, ((1,), (1,))), 0.0)
    mixer_high, mixer_low = split(mixer)
    mixed = fastdot(
        jnp.concatenate([mixer_high, mixer_low, mixer_high], axis=1),
        jnp.concatenate([owned_high, owned_high, owned_low], axis=0),
        ((1,), (0,)),
    )
    store(out_ref, mixed)
    one_of_each = cells(groups_n, rank, lambda row: row * per, lambda cell: cell)
    time_out_ref[...] = dot(one_of_each, basis) * math.sqrt(groups_n)


def mix(gram, time_factor, owned, groups_n):
    return pl.pallas_call(
        functools.partial(mix_kernel, groups_n),
        out_shape=(jax.ShapeDtypeStruct(owned.shape, F32), jax.ShapeDtypeStruct(time_factor.shape, F32)),
        compiler_params=SMALL,
        name="mix",
    )(gram, time_factor.T, owned)


def finish_kernel(scale, blocks, block_ref, mine_ref, other_ref, out_ref, made_ref, sems):
    rows = block_ref.shape[0] // blocks
    high, middle, low = split3(block_ref[...])
    left, left_more = jnp.concatenate([high, middle], axis=1), jnp.concatenate([high, low], axis=1)
    high, middle, low = split3(orth_factor(mine_ref[...] + other_ref[...]) * scale)
    both = jnp.concatenate([high, middle], axis=1)
    right, right_more = jnp.concatenate([both, both], axis=0), jnp.concatenate([low, high], axis=0)
    copies = []
    for i in range(blocks):
        take = pl.ds(i * rows, rows)
        part = slice(i * rows, (i + 1) * rows)
        made_ref[take] = by_stacked(left[part], right) + fastdot(left_more[part], right_more, ((1,), (0,)))
        copies.append(pltpu.make_async_copy(made_ref.at[take], out_ref.at[take], sems.at[i]))
        copies[-1].start()
    for copy in copies:
        copy.wait()


def finish(block, mine, other, scale, blocks=4):
    return pl.pallas_call(
        functools.partial(finish_kernel, scale, blocks),
        out_shape=jax.ShapeDtypeStruct(block.shape, F32),
        out_specs=pl.BlockSpec(memory_space=pl.ANY),
        scratch_shapes=[pltpu.VMEM(block.shape, F32), pltpu.SemaphoreType.DMA((blocks,))],
        compiler_params=SMALL,
        name="finish",
    )(block, mine, other)


def row_gram_kernel(block_ref, out_ref):
    high, low = split(block_ref[...])
    rank = high.shape[1]
    wide = fastdot(high, jnp.concatenate([high, low], axis=1), ((0,), (0,)))
    out_ref[...] = wide[:, :rank] + wide[:, rank:] + wide[:, rank:].T


def row_gram(block):
    rank = block.shape[1]
    return pl.pallas_call(row_gram_kernel, out_shape=jax.ShapeDtypeStruct((rank, rank), F32), compiler_params=SMALL, name="row_gram")(block)


def make_on_device(groups_n, reps):
    half_n = groups_n // 2
    halves = [[h * half_n + i for i in range(half_n)] for h in range(2)]
    across = [(i, (i + half_n) % groups_n) for i in range(groups_n)]
    swap = [(0, 1), (1, 0)]

    def all_to_all(value, parts, groups=None):
        shape = value.shape
        value = value.reshape((parts, shape[0] // parts) + shape[1:])
        value = lax.all_to_all(value, "grp", split_axis=0, concat_axis=0, tiled=True, axis_index_groups=groups)
        return value.reshape(shape)

    def to_owners(value):
        if len(value.shape) == 2:
            return all_to_all(value, groups_n)
        flat = value.reshape((groups_n * reps,) + value.shape[2:])
        return lax.all_to_all(flat, ("grp", "rep"), split_axis=0, concat_axis=0, tiled=True).reshape(value.shape)

    def on_device(snapshots, row_factor, time_factor):
        rows, cols = snapshots.shape[1:]
        rank = row_factor.shape[1]
        width = cols // reps
        fits = rank % (8 * groups_n) == 0 and width % (128 * reps) == 0
        packed = packed_shape(groups_n, reps if fits else 1, rank, width)
        send, far_high, far_low, held, both = project_first(snapshots[0], row_factor, width, packed)
        received = lax.ppermute(send, "rep", swap)
        summed, near_high, near_low = project_second(held, both, width, packed)
        summed = summed + received
        owned = to_owners(summed)
        devices = groups_n * reps
        if devices * groups_n * groups_n <= 1 << 20:
            grams = lax.all_to_all(
                small_gram(owned, groups_n, (devices, 1, groups_n * groups_n)),
                ("grp", "rep"),
                split_axis=0,
                concat_axis=0,
                tiled=True,
            )
        else:
            grams = lax.psum(small_gram(owned, groups_n, (groups_n, groups_n)), ("grp", "rep"))
        weights, new_time = mix(grams, time_factor, owned, groups_n)
        weight = to_owners(weights)
        other_weight = lax.ppermute(weight, "rep", swap)
        product = multiply(far_high, far_low, other_weight, multiply(near_high, near_low, weight))
        parts = all_to_all(product, half_n, halves)
        chunk = jnp.sum(parts.reshape(half_n, rows // half_n, rank), axis=0)
        chunk = chunk + lax.ppermute(chunk, "grp", across)
        block = all_to_all(jnp.tile(chunk, (half_n, 1)), half_n, halves)
        gram = row_gram(block)
        new_rows = finish(block, gram, lax.ppermute(gram, "rep", swap), math.sqrt(rows * reps))
        return (new_rows, new_time)

    return on_device


def solution(mesh):
    return jax.shard_map(
        make_on_device(mesh.shape["grp"], mesh.shape["rep"]),
        mesh=mesh,
        in_specs=(P("grp", "rep", None), P("rep", None), P()),
        out_specs=(P("rep", None), P()),
        check_vma=False,
    )
```

```python
import functools
import math

import jax
import jax.numpy as jnp
from jax import lax
from jax.experimental import pallas as pl
from jax.experimental.pallas import tpu as pltpu
from jax.sharding import PartitionSpec as P

STEPS = 8
SMALL = pltpu.CompilerParams(vmem_limit_bytes=16 << 20)
F32 = jnp.float32
BF16 = jnp.bfloat16
TINY = 1e-06


def dot(left, right, contract=((1,), (0,))):
    return lax.dot_general(
        left, right, (contract, ((), ())), precision=lax.Precision.HIGHEST, preferred_element_type=F32
    )


def fastdot(left, right, contract):
    return lax.dot_general(left, right, (contract, ((), ())), preferred_element_type=F32)


def split(value):
    high = value.astype(BF16)
    return high, (value - high.astype(F32)).astype(BF16)


def eye(size):
    return (lax.broadcasted_iota(jnp.int32, (size, size), 0) == lax.broadcasted_iota(jnp.int32, (size, size), 1)).astype(F32)


def split3(value):
    high = value.astype(BF16)
    rest = value - high.astype(F32)
    middle = rest.astype(BF16)
    return high, middle, (rest - middle.astype(F32)).astype(BF16)


def halves_of(value):
    high, low = split(value)
    return jnp.concatenate([high, low], axis=1)


def stack(right):
    both = halves_of(right)
    return jnp.concatenate([both, both], axis=0)


def by_stacked(left_halves, stacked):
    wide = fastdot(left_halves, stacked, ((1,), (0,)))
    size = stacked.shape[1] // 2
    return wide[:, :size] + wide[:, size:]


def tree_sum(terms):
    while len(terms) > 1:
        terms = [sum(terms[i : i + 2]) for i in range(0, len(terms), 2)]
    return terms[0]


def small_step(squared, factor, unit):
    size = unit.shape[0]
    columns = [jnp.broadcast_to(squared[:, k : k + 1], unit.shape) for k in range(size)]
    turn = 1.5 * unit - 0.5 * squared
    turn_columns = [1.5 * unit[:, k : k + 1] - 0.5 * columns[k] for k in range(size)]
    turn_squared = tree_sum([turn_columns[k] * turn[k : k + 1] for k in range(size)])
    factor = tree_sum([turn_columns[k] * factor[k : k + 1] for k in range(size)])
    return tree_sum([columns[k] * turn_squared[k : k + 1] for k in range(size)]), factor


def step(squared, factor, unit):
    if unit.shape[0] <= 16:
        return small_step(squared, factor, unit)
    turn = 1.5 * unit - 0.5 * squared
    if unit.shape[0] % 128:
        return dot(dot(squared, turn), turn), dot(factor, turn)
    rank = unit.shape[0]
    stacked = stack(squared)
    both = by_stacked(halves_of(jnp.concatenate([squared, factor], axis=0)), stacked)
    turn = 2.25 * unit - 1.5 * squared + 0.25 * both[:rank]
    return by_stacked(halves_of(turn), stacked), 1.5 * factor - 0.5 * both[rank:]


def orth_factor(gram):
    unit = eye(gram.shape[0])
    total = jnp.sum(gram * unit) + TINY
    squared = gram * (1.0 / total)
    factor = unit * lax.rsqrt(total)
    for step_index in range(STEPS):
        squared, factor = step(squared, factor, unit)
    return factor


def packed_shape(groups_n, cuts, rank, width):
    return (rank, width) if cuts == 1 else (groups_n, cuts, rank // groups_n, width // cuts)


def store(ref, value, add=False):
    if len(ref.shape) == 2:
        ref[...] = ref[...] + value if add else value
        return
    groups_n, cuts, per, piece = ref.shape
    for k in range(cuts):
        part = value[:, k * piece : (k + 1) * piece].reshape(groups_n, per, piece)
        ref[:, k] = ref[:, k] + part if add else part


def load(ref):
    if len(ref.shape) == 2:
        return ref[...]
    groups_n, cuts, per, piece = ref.shape
    return jnp.concatenate([ref[:, k].reshape(groups_n * per, piece) for k in range(cuts)], axis=1)


def project_block(image_high, image_low, factor_both):
    rank = factor_both.shape[1] // 2
    wide = fastdot(factor_both, image_high, ((0,), (0,)))
    return wide[:rank] + wide[rank:] + fastdot(factor_both[:, :rank], image_low, ((0,), (0,)))


def columns_of(part, width):
    return pl.ds(pl.multiple_of(lax.rem(lax.axis_index("rep") + part, lax.axis_size("rep")) * width, width), width)


def first_kernel(image_ref, factor_ref, out_ref, high_ref, low_ref, held_ref, both_ref, fetched_ref, sems, factor_sem):
    blocks = sems.shape[0]
    rows, width = high_ref.shape
    block = rows // blocks
    copies = []
    factor_copy = pltpu.make_async_copy(factor_ref, fetched_ref, factor_sem)
    factor_copy.start()
    for i in range(blocks):
        take = pl.ds(i * block, block)
        copies.append(pltpu.make_async_copy(image_ref.at[take], held_ref.at[take], sems.at[i]))
        copies[-1].start()
    factor_copy.wait()
    both_ref[...] = halves_of(fetched_ref[...])
    columns = columns_of(1, width)
    for i in range(blocks):
        copies[i].wait()
        take = pl.ds(i * block, block)
        high, low = split(held_ref[take, columns])
        high_ref[take] = high
        low_ref[take] = low
        value = project_block(high, low, both_ref[take])
        store(out_ref, value, add=i > 0)


def project_first(image, row_factor, width, packed, blocks=2):
    rows, rank = row_factor.shape
    return pl.pallas_call(
        first_kernel,
        in_specs=[pl.BlockSpec(memory_space=pl.ANY), pl.BlockSpec(memory_space=pl.ANY)],
        out_shape=(
            jax.ShapeDtypeStruct(packed, F32),
            jax.ShapeDtypeStruct((rows, width), BF16),
            jax.ShapeDtypeStruct((rows, width), BF16),
            jax.ShapeDtypeStruct(image.shape, F32),
            jax.ShapeDtypeStruct((rows, 2 * rank), BF16),
        ),
        scratch_shapes=[
            pltpu.VMEM((rows, rank), F32),
            pltpu.SemaphoreType.DMA((blocks,)),
            pltpu.SemaphoreType.DMA,
        ],
        compiler_params=SMALL,
        name="project_first",
    )(
        pltpu.with_memory_space_constraint(image, pltpu.HBM),
        pltpu.with_memory_space_constraint(row_factor, pltpu.HBM),
    )


def second_kernel(blocks, held_ref, both_ref, out_ref, high_ref, low_ref):
    rows, width = high_ref.shape
    block = rows // blocks
    columns = columns_of(0, width)
    total = None
    for i in range(blocks):
        take = pl.ds(i * block, block)
        high, low = split(held_ref[take, columns])
        high_ref[take] = high
        low_ref[take] = low
        value = project_block(high, low, both_ref[take])
        total = value if total is None else total + value
    store(out_ref, total)


def project_second(held, both, width, packed, blocks=4):
    rows, rank = both.shape[0], both.shape[1] // 2
    return pl.pallas_call(
        functools.partial(second_kernel, blocks),
        out_shape=(
            jax.ShapeDtypeStruct(packed, F32),
            jax.ShapeDtypeStruct((rows, width), BF16),
            jax.ShapeDtypeStruct((rows, width), BF16),
        ),
        cost_estimate=pl.CostEstimate(
            flops=6 * rows * width * rank, bytes_accessed=4 * rows * (width + rank), transcendentals=0
        ),
        compiler_params=SMALL,
        name="project_second",
    )(held, both)


def product_kernel(blocks, high_ref, low_ref, weight_ref, *refs):
    out_ref = refs[-1]
    weight_high, weight_low = split(load(weight_ref))
    rank = weight_high.shape[0]
    both = jnp.concatenate([weight_high, weight_low], axis=0)
    block = out_ref.shape[0] // blocks
    for i in range(blocks):
        take = pl.ds(i * block, block)
        wide = fastdot(high_ref[take], both, ((1,), (1,)))
        value = wide[:, :rank] + wide[:, rank:] + fastdot(low_ref[take], weight_high, ((1,), (1,)))
        if len(refs) > 1:
            value = value + refs[0][take]
        out_ref[take] = value


def multiply(high, low, weight, start=None, blocks=4):
    rows, width = high.shape
    rank = weight.size // width
    more = () if start is None else (start,)
    return pl.pallas_call(
        functools.partial(product_kernel, blocks),
        out_shape=jax.ShapeDtypeStruct((rows, rank), F32),
        cost_estimate=pl.CostEstimate(
            flops=6 * rows * width * rank, bytes_accessed=4 * rows * (width + rank), transcendentals=0
        ),
        compiler_params=SMALL,
        name="multiply",
    )(high, low, weight, *more)


def cells(rows, count, row_of, cell_of):
    row = row_of(lax.broadcasted_iota(jnp.int32, (rows, count), 0))
    return (row == cell_of(lax.broadcasted_iota(jnp.int32, (rows, count), 1))).astype(F32)


def spread(groups_n, rank):
    per = rank // groups_n
    return cells(rank, groups_n, lambda row: row // per, lambda cell: cell)


def same_slot(groups_n, rank):
    per = rank // groups_n
    return cells(rank, rank, lambda row: row % per, lambda cell: cell % per) > 0.5


def gram_kernel(groups_n, owned_ref, out_ref):
    high, low = split(load(owned_ref))
    rank = high.shape[0]
    per = rank // groups_n
    wide = fastdot(high, jnp.concatenate([high, low], axis=0), ((1,), (1,)))
    full = wide[:, :rank] + wide[:, rank:] + wide[:, rank:].T
    full = jnp.where(same_slot(groups_n, rank), full, 0.0)
    if len(out_ref.shape) == 2:
        fold = spread(groups_n, rank)
        out_ref[...] = dot(dot(fold, full, ((0,), (0,))), fold)
    else:
        count = out_ref.shape[2]
        columns = cells(rank, count, lambda row: row // per, lambda cell: cell % groups_n).astype(BF16)
        folded = fastdot(
            jnp.concatenate(split3(full), axis=1), jnp.concatenate([columns, columns, columns], axis=0), ((1,), (0,))
        )
        rows = cells(rank, count, lambda row: row // per, lambda cell: cell // groups_n)
        flat = jnp.sum(rows * folded, axis=0, keepdims=True)
        out_ref[...] = jnp.broadcast_to(flat[None], out_ref.shape)


def small_gram(owned, groups_n, shape):
    return pl.pallas_call(
        functools.partial(gram_kernel, groups_n),
        out_shape=jax.ShapeDtypeStruct(shape, F32),
        compiler_params=SMALL,
        name="small_gram",
    )(owned)


def mix_kernel(groups_n, gram_ref, time_ref, owned_ref, out_ref, time_out_ref):
    owned_high, owned_low = split(load(owned_ref))
    rank = owned_high.shape[0]
    per = rank // groups_n
    if len(gram_ref.shape) == 2:
        fold = spread(groups_n, rank)
        start = dot(fold, dot(gram_ref[...], time_ref[...], ((1,), (1,))))
        turned = dot(dot(time_ref[...], gram_ref[...], ((1,), (1,))), fold, ((1,), (1,)))
    else:
        count = gram_ref.shape[2]
        flat = jnp.sum(gram_ref[...], axis=0)
        rows = cells(rank, count, lambda row: row // per, lambda cell: cell // groups_n) * flat
        columns = dot(time_ref[...], cells(groups_n, count, lambda row: row, lambda cell: cell % groups_n))
        start = dot(rows, columns, ((1,), (1,)))
        turned = dot(columns, rows, ((1,), (1,)))
    factor = orth_factor(dot(turned, start) * (1.0 / per))
    size = factor.shape[0]
    if size <= 16:
        basis = tree_sum([start[:, k : k + 1] * factor[k : k + 1] for k in range(size)])
    else:
        basis = dot(start, factor)
    mixer = jnp.where(same_slot(groups_n, rank), dot(basis, basis, ((1,), (1,))), 0.0)
    mixer_high, mixer_low = split(mixer)
    mixed = fastdot(
        jnp.concatenate([mixer_high, mixer_low, mixer_high], axis=1),
        jnp.concatenate([owned_high, owned_high, owned_low], axis=0),
        ((1,), (0,)),
    )
    store(out_ref, mixed)
    one_of_each = cells(groups_n, rank, lambda row: row * per, lambda cell: cell)
    time_out_ref[...] = dot(one_of_each, basis) * math.sqrt(groups_n)


def mix(gram, time_factor, owned, groups_n):
    return pl.pallas_call(
        functools.partial(mix_kernel, groups_n),
        out_shape=(jax.ShapeDtypeStruct(owned.shape, F32), jax.ShapeDtypeStruct(time_factor.shape, F32)),
        compiler_params=SMALL,
        name="mix",
    )(gram, time_factor.T, owned)


def finish_kernel(scale, blocks, block_ref, mine_ref, other_ref, out_ref, made_ref, sems):
    rows = block_ref.shape[0] // blocks
    high, middle, low = split3(block_ref[...])
    left, left_more = jnp.concatenate([high, middle], axis=1), jnp.concatenate([high, low], axis=1)
    high, middle, low = split3(orth_factor(mine_ref[...] + other_ref[...]) * scale)
    both = jnp.concatenate([high, middle], axis=1)
    right, right_more = jnp.concatenate([both, both], axis=0), jnp.concatenate([low, high], axis=0)
    copies = []
    for i in range(blocks):
        take = pl.ds(i * rows, rows)
        part = slice(i * rows, (i + 1) * rows)
        made_ref[take] = by_stacked(left[part], right) + fastdot(left_more[part], right_more, ((1,), (0,)))
        copies.append(pltpu.make_async_copy(made_ref.at[take], out_ref.at[take], sems.at[i]))
        copies[-1].start()
    for copy in copies:
        copy.wait()


def finish(block, mine, other, scale, blocks=4):
    return pl.pallas_call(
        functools.partial(finish_kernel, scale, blocks),
        out_shape=jax.ShapeDtypeStruct(block.shape, F32),
        out_specs=pl.BlockSpec(memory_space=pl.ANY),
        scratch_shapes=[pltpu.VMEM(block.shape, F32), pltpu.SemaphoreType.DMA((blocks,))],
        compiler_params=SMALL,
        name="finish",
    )(block, mine, other)


def row_gram_kernel(block_ref, out_ref):
    high, low = split(block_ref[...])
    rank = high.shape[1]
    wide = fastdot(high, jnp.concatenate([high, low], axis=1), ((0,), (0,)))
    out_ref[...] = wide[:, :rank] + wide[:, rank:] + wide[:, rank:].T


def row_gram(block):
    rank = block.shape[1]
    return pl.pallas_call(row_gram_kernel, out_shape=jax.ShapeDtypeStruct((rank, rank), F32), compiler_params=SMALL, name="row_gram")(block)


def make_on_device(groups_n, reps):
    half_n = groups_n // 2
    halves = [[h * half_n + i for i in range(half_n)] for h in range(2)]
    across = [(i, (i + half_n) % groups_n) for i in range(groups_n)]
    swap = [(0, 1), (1, 0)]

    def all_to_all(value, parts, groups=None):
        shape = value.shape
        value = value.reshape((parts, shape[0] // parts) + shape[1:])
        value = lax.all_to_all(value, "grp", split_axis=0, concat_axis=0, tiled=True, axis_index_groups=groups)
        return value.reshape(shape)

    def to_owners(value):
        if len(value.shape) == 2:
            return all_to_all(value, groups_n)
        flat = value.reshape((groups_n * reps,) + value.shape[2:])
        return lax.all_to_all(flat, ("grp", "rep"), split_axis=0, concat_axis=0, tiled=True).reshape(value.shape)

    def on_device(snapshots, row_factor, time_factor):
        rows, cols = snapshots.shape[1:]
        rank = row_factor.shape[1]
        width = cols // reps
        fits = rank % (8 * groups_n) == 0 and width % (128 * reps) == 0
        packed = packed_shape(groups_n, reps if fits else 1, rank, width)
        send, far_high, far_low, held, both = project_first(snapshots[0], row_factor, width, packed)
        received = lax.ppermute(send, "rep", swap)
        summed, near_high, near_low = project_second(held, both, width, packed)
        summed = summed + received
        owned = to_owners(summed)
        devices = groups_n * reps
        if devices * groups_n * groups_n <= 1 << 20:
            grams = lax.all_to_all(
                small_gram(owned, groups_n, (devices, 1, groups_n * groups_n)),
                ("grp", "rep"),
                split_axis=0,
                concat_axis=0,
                tiled=True,
            )
        else:
            grams = lax.psum(small_gram(owned, groups_n, (groups_n, groups_n)), ("grp", "rep"))
        weights, new_time = mix(grams, time_factor, owned, groups_n)
        weight = to_owners(weights)
        other_weight = lax.ppermute(weight, "rep", swap)
        product = multiply(far_high, far_low, other_weight, multiply(near_high, near_low, weight))
        parts = all_to_all(product, half_n, halves)
        chunk = jnp.sum(parts.reshape(half_n, rows // half_n, rank), axis=0)
        chunk = chunk + lax.ppermute(chunk, "grp", across)
        block = all_to_all(jnp.tile(chunk, (half_n, 1)), half_n, halves)
        gram = row_gram(block)
        new_rows = finish(block, gram, lax.ppermute(gram, "rep", swap), math.sqrt(rows * reps))
        return (new_rows, new_time)

    return on_device


def solution(mesh):
    return jax.shard_map(
        make_on_device(mesh.shape["grp"], mesh.shape["rep"]),
        mesh=mesh,
        in_specs=(P("grp", "rep", None), P("rep", None), P()),
        out_specs=(P("rep", None), P()),
        check_vma=False,
    )
```

```python
import functools
import math

import jax
import jax.numpy as jnp
from jax import lax
from jax.experimental import pallas as pl
from jax.experimental.pallas import tpu as pltpu
from jax.sharding import PartitionSpec as P

STEPS = 8
SMALL = pltpu.CompilerParams(vmem_limit_bytes=16 << 20)
F32 = jnp.float32
BF16 = jnp.bfloat16
TINY = 1e-06


def dot(left, right, contract=((1,), (0,))):
    return lax.dot_general(
        left, right, (contract, ((), ())), precision=lax.Precision.HIGHEST, preferred_element_type=F32
    )


def fastdot(left, right, contract):
    return lax.dot_general(left, right, (contract, ((), ())), preferred_element_type=F32)


def split(value):
    high = value.astype(BF16)
    return high, (value - high.astype(F32)).astype(BF16)


def eye(size):
    return (lax.broadcasted_iota(jnp.int32, (size, size), 0) == lax.broadcasted_iota(jnp.int32, (size, size), 1)).astype(F32)


def split3(value):
    high = value.astype(BF16)
    rest = value - high.astype(F32)
    middle = rest.astype(BF16)
    return high, middle, (rest - middle.astype(F32)).astype(BF16)


def halves_of(value):
    high, low = split(value)
    return jnp.concatenate([high, low], axis=1)


def stack(right):
    both = halves_of(right)
    return jnp.concatenate([both, both], axis=0)


def by_stacked(left_halves, stacked):
    wide = fastdot(left_halves, stacked, ((1,), (0,)))
    size = stacked.shape[1] // 2
    return wide[:, :size] + wide[:, size:]


def tree_sum(terms):
    while len(terms) > 1:
        terms = [sum(terms[i : i + 2]) for i in range(0, len(terms), 2)]
    return terms[0]


def small_step(squared, factor, unit):
    size = unit.shape[0]
    columns = [jnp.broadcast_to(squared[:, k : k + 1], unit.shape) for k in range(size)]
    turn = 1.5 * unit - 0.5 * squared
    turn_columns = [1.5 * unit[:, k : k + 1] - 0.5 * columns[k] for k in range(size)]
    turn_squared = tree_sum([turn_columns[k] * turn[k : k + 1] for k in range(size)])
    factor = tree_sum([turn_columns[k] * factor[k : k + 1] for k in range(size)])
    return tree_sum([columns[k] * turn_squared[k : k + 1] for k in range(size)]), factor


def step(squared, factor, unit):
    if unit.shape[0] <= 16:
        return small_step(squared, factor, unit)
    turn = 1.5 * unit - 0.5 * squared
    if unit.shape[0] % 128:
        return dot(dot(squared, turn), turn), dot(factor, turn)
    rank = unit.shape[0]
    stacked = stack(squared)
    both = by_stacked(halves_of(jnp.concatenate([squared, factor], axis=0)), stacked)
    turn = 2.25 * unit - 1.5 * squared + 0.25 * both[:rank]
    return by_stacked(halves_of(turn), stacked), 1.5 * factor - 0.5 * both[rank:]


def orth_factor(gram):
    unit = eye(gram.shape[0])
    total = jnp.sum(gram * unit) + TINY
    squared = gram * (1.0 / total)
    factor = unit * lax.rsqrt(total)
    for step_index in range(STEPS):
        squared, factor = step(squared, factor, unit)
    return factor


def packed_shape(groups_n, cuts, rank, width):
    return (rank, width) if cuts == 1 else (groups_n, cuts, rank // groups_n, width // cuts)


def store(ref, value, add=False):
    if len(ref.shape) == 2:
        ref[...] = ref[...] + value if add else value
        return
    groups_n, cuts, per, piece = ref.shape
    for k in range(cuts):
        part = value[:, k * piece : (k + 1) * piece].reshape(groups_n, per, piece)
        ref[:, k] = ref[:, k] + part if add else part


def load(ref):
    if len(ref.shape) == 2:
        return ref[...]
    groups_n, cuts, per, piece = ref.shape
    return jnp.concatenate([ref[:, k].reshape(groups_n * per, piece) for k in range(cuts)], axis=1)


def project_block(image_high, image_low, factor_both):
    rank = factor_both.shape[1] // 2
    wide = fastdot(factor_both, image_high, ((0,), (0,)))
    return wide[:rank] + wide[rank:] + fastdot(factor_both[:, :rank], image_low, ((0,), (0,)))


def columns_of(part, width):
    return pl.ds(pl.multiple_of(lax.rem(lax.axis_index("rep") + part, lax.axis_size("rep")) * width, width), width)


def first_kernel(image_ref, factor_ref, out_ref, high_ref, low_ref, held_ref, both_ref, fetched_ref, sems, factor_sem):
    blocks = sems.shape[0]
    rows, width = high_ref.shape
    block = rows // blocks
    copies = []
    factor_copy = pltpu.make_async_copy(factor_ref, fetched_ref, factor_sem)
    factor_copy.start()
    for i in range(blocks):
        take = pl.ds(i * block, block)
        copies.append(pltpu.make_async_copy(image_ref.at[take], held_ref.at[take], sems.at[i]))
        copies[-1].start()
    factor_copy.wait()
    both_ref[...] = halves_of(fetched_ref[...])
    columns = columns_of(1, width)
    for i in range(blocks):
        copies[i].wait()
        take = pl.ds(i * block, block)
        high, low = split(held_ref[take, columns])
        high_ref[take] = high
        low_ref[take] = low
        value = project_block(high, low, both_ref[take])
        store(out_ref, value, add=i > 0)


def project_first(image, row_factor, width, packed, blocks=2):
    rows, rank = row_factor.shape
    return pl.pallas_call(
        first_kernel,
        in_specs=[pl.BlockSpec(memory_space=pl.ANY), pl.BlockSpec(memory_space=pl.ANY)],
        out_shape=(
            jax.ShapeDtypeStruct(packed, F32),
            jax.ShapeDtypeStruct((rows, width), BF16),
            jax.ShapeDtypeStruct((rows, width), BF16),
            jax.ShapeDtypeStruct(image.shape, F32),
            jax.ShapeDtypeStruct((rows, 2 * rank), BF16),
        ),
        scratch_shapes=[
            pltpu.VMEM((rows, rank), F32),
            pltpu.SemaphoreType.DMA((blocks,)),
            pltpu.SemaphoreType.DMA,
        ],
        compiler_params=SMALL,
        name="project_first",
    )(
        pltpu.with_memory_space_constraint(image, pltpu.HBM),
        pltpu.with_memory_space_constraint(row_factor, pltpu.HBM),
    )


def second_kernel(blocks, held_ref, both_ref, out_ref, high_ref, low_ref):
    rows, width = high_ref.shape
    block = rows // blocks
    columns = columns_of(0, width)
    total = None
    for i in range(blocks):
        take = pl.ds(i * block, block)
        high, low = split(held_ref[take, columns])
        high_ref[take] = high
        low_ref[take] = low
        value = project_block(high, low, both_ref[take])
        total = value if total is None else total + value
    store(out_ref, total)


def project_second(held, both, width, packed, blocks=4):
    rows, rank = both.shape[0], both.shape[1] // 2
    return pl.pallas_call(
        functools.partial(second_kernel, blocks),
        out_shape=(
            jax.ShapeDtypeStruct(packed, F32),
            jax.ShapeDtypeStruct((rows, width), BF16),
            jax.ShapeDtypeStruct((rows, width), BF16),
        ),
        cost_estimate=pl.CostEstimate(
            flops=6 * rows * width * rank, bytes_accessed=4 * rows * (width + rank), transcendentals=0
        ),
        compiler_params=SMALL,
        name="project_second",
    )(held, both)


def product_kernel(blocks, high_ref, low_ref, weight_ref, *refs):
    out_ref = refs[-1]
    weight_high, weight_low = split(load(weight_ref))
    rank = weight_high.shape[0]
    both = jnp.concatenate([weight_high, weight_low], axis=0)
    block = out_ref.shape[0] // blocks
    for i in range(blocks):
        take = pl.ds(i * block, block)
        wide = fastdot(high_ref[take], both, ((1,), (1,)))
        value = wide[:, :rank] + wide[:, rank:] + fastdot(low_ref[take], weight_high, ((1,), (1,)))
        if len(refs) > 1:
            value = value + refs[0][take]
        out_ref[take] = value


def multiply(high, low, weight, start=None, blocks=4):
    rows, width = high.shape
    rank = weight.size // width
    more = () if start is None else (start,)
    return pl.pallas_call(
        functools.partial(product_kernel, blocks),
        out_shape=jax.ShapeDtypeStruct((rows, rank), F32),
        cost_estimate=pl.CostEstimate(
            flops=6 * rows * width * rank, bytes_accessed=4 * rows * (width + rank), transcendentals=0
        ),
        compiler_params=SMALL,
        name="multiply",
    )(high, low, weight, *more)


def cells(rows, count, row_of, cell_of):
    row = row_of(lax.broadcasted_iota(jnp.int32, (rows, count), 0))
    return (row == cell_of(lax.broadcasted_iota(jnp.int32, (rows, count), 1))).astype(F32)


def spread(groups_n, rank):
    per = rank // groups_n
    return cells(rank, groups_n, lambda row: row // per, lambda cell: cell)


def same_slot(groups_n, rank):
    per = rank // groups_n
    return cells(rank, rank, lambda row: row % per, lambda cell: cell % per) > 0.5


def gram_kernel(groups_n, owned_ref, out_ref):
    high, low = split(load(owned_ref))
    rank = high.shape[0]
    per = rank // groups_n
    wide = fastdot(high, jnp.concatenate([high, low], axis=0), ((1,), (1,)))
    full = wide[:, :rank] + wide[:, rank:] + wide[:, rank:].T
    full = jnp.where(same_slot(groups_n, rank), full, 0.0)
    if len(out_ref.shape) == 2:
        fold = spread(groups_n, rank)
        out_ref[...] = dot(dot(fold, full, ((0,), (0,))), fold)
    else:
        count = out_ref.shape[2]
        columns = cells(rank, count, lambda row: row // per, lambda cell: cell % groups_n).astype(BF16)
        folded = fastdot(
            jnp.concatenate(split3(full), axis=1), jnp.concatenate([columns, columns, columns], axis=0), ((1,), (0,))
        )
        rows = cells(rank, count, lambda row: row // per, lambda cell: cell // groups_n)
        flat = jnp.sum(rows * folded, axis=0, keepdims=True)
        out_ref[...] = jnp.broadcast_to(flat[None], out_ref.shape)


def small_gram(owned, groups_n, shape):
    return pl.pallas_call(
        functools.partial(gram_kernel, groups_n),
        out_shape=jax.ShapeDtypeStruct(shape, F32),
        compiler_params=SMALL,
        name="small_gram",
    )(owned)


def mix_kernel(groups_n, gram_ref, time_ref, owned_ref, out_ref, time_out_ref):
    owned_high, owned_low = split(load(owned_ref))
    rank = owned_high.shape[0]
    per = rank // groups_n
    if len(gram_ref.shape) == 2:
        fold = spread(groups_n, rank)
        start = dot(fold, dot(gram_ref[...], time_ref[...], ((1,), (1,))))
        turned = dot(dot(time_ref[...], gram_ref[...], ((1,), (1,))), fold, ((1,), (1,)))
    else:
        count = gram_ref.shape[2]
        flat = jnp.sum(gram_ref[...], axis=0)
        rows = cells(rank, count, lambda row: row // per, lambda cell: cell // groups_n) * flat
        columns = dot(time_ref[...], cells(groups_n, count, lambda row: row, lambda cell: cell % groups_n))
        start = dot(rows, columns, ((1,), (1,)))
        turned = dot(columns, rows, ((1,), (1,)))
    factor = orth_factor(dot(turned, start) * (1.0 / per))
    size = factor.shape[0]
    if size <= 16:
        basis = tree_sum([start[:, k : k + 1] * factor[k : k + 1] for k in range(size)])
        basis_turned = tree_sum([factor[:, k : k + 1] * turned[k : k + 1] for k in range(size)])
        outer = tree_sum([basis[:, k : k + 1] * basis_turned[k : k + 1] for k in range(size)])
    else:
        basis = dot(start, factor)
        outer = dot(basis, basis, ((1,), (1,)))
    mixer = jnp.where(same_slot(groups_n, rank), outer, 0.0)
    mixer_high, mixer_low = split(mixer)
    mixed = fastdot(
        jnp.concatenate([mixer_high, mixer_low, mixer_high], axis=1),
        jnp.concatenate([owned_high, owned_high, owned_low], axis=0),
        ((1,), (0,)),
    )
    store(out_ref, mixed)
    one_of_each = cells(groups_n, rank, lambda row: row * per, lambda cell: cell)
    time_out_ref[...] = dot(one_of_each, basis) * math.sqrt(groups_n)


def mix(gram, time_factor, owned, groups_n):
    return pl.pallas_call(
        functools.partial(mix_kernel, groups_n),
        out_shape=(jax.ShapeDtypeStruct(owned.shape, F32), jax.ShapeDtypeStruct(time_factor.shape, F32)),
        compiler_params=SMALL,
        name="mix",
    )(gram, time_factor.T, owned)


def finish_kernel(scale, blocks, block_ref, mine_ref, other_ref, out_ref, made_ref, sems):
    rows = block_ref.shape[0] // blocks
    high, middle, low = split3(block_ref[...])
    left, left_more = jnp.concatenate([high, middle], axis=1), jnp.concatenate([high, low], axis=1)
    high, middle, low = split3(orth_factor(mine_ref[...] + other_ref[...]) * scale)
    both = jnp.concatenate([high, middle], axis=1)
    right, right_more = jnp.concatenate([both, both], axis=0), jnp.concatenate([low, high], axis=0)
    copies = []
    for i in range(blocks):
        take = pl.ds(i * rows, rows)
        part = slice(i * rows, (i + 1) * rows)
        made_ref[take] = by_stacked(left[part], right) + fastdot(left_more[part], right_more, ((1,), (0,)))
        copies.append(pltpu.make_async_copy(made_ref.at[take], out_ref.at[take], sems.at[i]))
        copies[-1].start()
    for copy in copies:
        copy.wait()


def finish(block, mine, other, scale, blocks=4):
    return pl.pallas_call(
        functools.partial(finish_kernel, scale, blocks),
        out_shape=jax.ShapeDtypeStruct(block.shape, F32),
        out_specs=pl.BlockSpec(memory_space=pl.ANY),
        scratch_shapes=[pltpu.VMEM(block.shape, F32), pltpu.SemaphoreType.DMA((blocks,))],
        compiler_params=SMALL,
        name="finish",
    )(block, mine, other)


def row_gram_kernel(block_ref, out_ref):
    high, low = split(block_ref[...])
    rank = high.shape[1]
    wide = fastdot(high, jnp.concatenate([high, low], axis=1), ((0,), (0,)))
    out_ref[...] = wide[:, :rank] + wide[:, rank:] + wide[:, rank:].T


def row_gram(block):
    rank = block.shape[1]
    return pl.pallas_call(row_gram_kernel, out_shape=jax.ShapeDtypeStruct((rank, rank), F32), compiler_params=SMALL, name="row_gram")(block)


def make_on_device(groups_n, reps):
    half_n = groups_n // 2
    halves = [[h * half_n + i for i in range(half_n)] for h in range(2)]
    across = [(i, (i + half_n) % groups_n) for i in range(groups_n)]
    swap = [(0, 1), (1, 0)]

    def all_to_all(value, parts, groups=None):
        shape = value.shape
        value = value.reshape((parts, shape[0] // parts) + shape[1:])
        value = lax.all_to_all(value, "grp", split_axis=0, concat_axis=0, tiled=True, axis_index_groups=groups)
        return value.reshape(shape)

    def to_owners(value):
        if len(value.shape) == 2:
            return all_to_all(value, groups_n)
        flat = value.reshape((groups_n * reps,) + value.shape[2:])
        return lax.all_to_all(flat, ("grp", "rep"), split_axis=0, concat_axis=0, tiled=True).reshape(value.shape)

    def on_device(snapshots, row_factor, time_factor):
        rows, cols = snapshots.shape[1:]
        rank = row_factor.shape[1]
        width = cols // reps
        fits = rank % (8 * groups_n) == 0 and width % (128 * reps) == 0
        packed = packed_shape(groups_n, reps if fits else 1, rank, width)
        send, far_high, far_low, held, both = project_first(snapshots[0], row_factor, width, packed)
        received = lax.ppermute(send, "rep", swap)
        summed, near_high, near_low = project_second(held, both, width, packed)
        summed = summed + received
        owned = to_owners(summed)
        devices = groups_n * reps
        if devices * groups_n * groups_n <= 1 << 20:
            grams = lax.all_to_all(
                small_gram(owned, groups_n, (devices, 1, groups_n * groups_n)),
                ("grp", "rep"),
                split_axis=0,
                concat_axis=0,
                tiled=True,
            )
        else:
            grams = lax.psum(small_gram(owned, groups_n, (groups_n, groups_n)), ("grp", "rep"))
        weights, new_time = mix(grams, time_factor, owned, groups_n)
        weight = to_owners(weights)
        other_weight = lax.ppermute(weight, "rep", swap)
        product = multiply(far_high, far_low, other_weight, multiply(near_high, near_low, weight))
        parts = all_to_all(product, half_n, halves)
        chunk = jnp.sum(parts.reshape(half_n, rows // half_n, rank), axis=0)
        chunk = chunk + lax.ppermute(chunk, "grp", across)
        block = all_to_all(jnp.tile(chunk, (half_n, 1)), half_n, halves)
        gram = row_gram(block)
        new_rows = finish(block, gram, lax.ppermute(gram, "rep", swap), math.sqrt(rows * reps))
        return (new_rows, new_time)

    return on_device


def solution(mesh):
    return jax.shard_map(
        make_on_device(mesh.shape["grp"], mesh.shape["rep"]),
        mesh=mesh,
        in_specs=(P("grp", "rep", None), P("rep", None), P()),
        out_specs=(P("rep", None), P()),
        check_vma=False,
    )
```

```python
import functools
import math

import jax
import jax.numpy as jnp
from jax import lax
from jax.experimental import pallas as pl
from jax.experimental.pallas import tpu as pltpu
from jax.sharding import PartitionSpec as P

STEPS = 8
SMALL = pltpu.CompilerParams(vmem_limit_bytes=16 << 20)
F32 = jnp.float32
BF16 = jnp.bfloat16
TINY = 1e-06


def dot(left, right, contract=((1,), (0,))):
    return lax.dot_general(
        left, right, (contract, ((), ())), precision=lax.Precision.HIGHEST, preferred_element_type=F32
    )


def fastdot(left, right, contract):
    return lax.dot_general(left, right, (contract, ((), ())), preferred_element_type=F32)


def split(value):
    high = value.astype(BF16)
    return high, (value - high.astype(F32)).astype(BF16)


def eye(size):
    return (lax.broadcasted_iota(jnp.int32, (size, size), 0) == lax.broadcasted_iota(jnp.int32, (size, size), 1)).astype(F32)


def split3(value):
    high = value.astype(BF16)
    rest = value - high.astype(F32)
    middle = rest.astype(BF16)
    return high, middle, (rest - middle.astype(F32)).astype(BF16)


def halves_of(value):
    high, low = split(value)
    return jnp.concatenate([high, low], axis=1)


def stack(right):
    both = halves_of(right)
    return jnp.concatenate([both, both], axis=0)


def by_stacked(left_halves, stacked):
    wide = fastdot(left_halves, stacked, ((1,), (0,)))
    size = stacked.shape[1] // 2
    return wide[:, :size] + wide[:, size:]


def tree_sum(terms):
    while len(terms) > 1:
        terms = [sum(terms[i : i + 2]) for i in range(0, len(terms), 2)]
    return terms[0]


def small_step(squared, factor, unit):
    size = unit.shape[0]
    columns = [jnp.broadcast_to(squared[:, k : k + 1], unit.shape) for k in range(size)]
    turn_columns = [1.5 * unit[:, k : k + 1] - 0.5 * columns[k] for k in range(size)]
    turn_rows = [1.5 * unit[k : k + 1] - 0.5 * jnp.broadcast_to(squared[k : k + 1], unit.shape) for k in range(size)]
    turn_squared = tree_sum([turn_columns[k] * turn_rows[k] for k in range(size)])
    factor = tree_sum([turn_columns[k] * factor[k : k + 1] for k in range(size)])
    return tree_sum([columns[k] * turn_squared[k : k + 1] for k in range(size)]), factor


def step(squared, factor, unit):
    if unit.shape[0] <= 16:
        return small_step(squared, factor, unit)
    turn = 1.5 * unit - 0.5 * squared
    if unit.shape[0] % 128:
        return dot(dot(squared, turn), turn), dot(factor, turn)
    rank = unit.shape[0]
    stacked = stack(squared)
    both = by_stacked(halves_of(jnp.concatenate([squared, factor], axis=0)), stacked)
    turn = 2.25 * unit - 1.5 * squared + 0.25 * both[:rank]
    return by_stacked(halves_of(turn), stacked), 1.5 * factor - 0.5 * both[rank:]


def orth_factor(gram):
    unit = eye(gram.shape[0])
    total = jnp.sum(gram * unit) + TINY
    squared = gram * (1.0 / total)
    factor = unit * lax.rsqrt(total)
    for step_index in range(STEPS):
        squared, factor = step(squared, factor, unit)
    return factor


def packed_shape(groups_n, cuts, rank, width):
    return (rank, width) if cuts == 1 else (groups_n, cuts, rank // groups_n, width // cuts)


def store(ref, value, add=False):
    if len(ref.shape) == 2:
        ref[...] = ref[...] + value if add else value
        return
    groups_n, cuts, per, piece = ref.shape
    for k in range(cuts):
        part = value[:, k * piece : (k + 1) * piece].reshape(groups_n, per, piece)
        ref[:, k] = ref[:, k] + part if add else part


def load(ref):
    if len(ref.shape) == 2:
        return ref[...]
    groups_n, cuts, per, piece = ref.shape
    return jnp.concatenate([ref[:, k].reshape(groups_n * per, piece) for k in range(cuts)], axis=1)


def project_block(image_high, image_low, factor_both):
    rank = factor_both.shape[1] // 2
    wide = fastdot(factor_both, image_high, ((0,), (0,)))
    return wide[:rank] + wide[rank:] + fastdot(factor_both[:, :rank], image_low, ((0,), (0,)))


def columns_of(part, width):
    return pl.ds(pl.multiple_of(lax.rem(lax.axis_index("rep") + part, lax.axis_size("rep")) * width, width), width)


def first_kernel(image_ref, factor_ref, out_ref, high_ref, low_ref, held_ref, both_ref, fetched_ref, sems, factor_sem):
    blocks = sems.shape[0]
    rows, width = high_ref.shape
    block = rows // blocks
    copies = []
    factor_copy = pltpu.make_async_copy(factor_ref, fetched_ref, factor_sem)
    factor_copy.start()
    for i in range(blocks):
        take = pl.ds(i * block, block)
        copies.append(pltpu.make_async_copy(image_ref.at[take], held_ref.at[take], sems.at[i]))
        copies[-1].start()
    factor_copy.wait()
    both_ref[...] = halves_of(fetched_ref[...])
    columns = columns_of(1, width)
    for i in range(blocks):
        copies[i].wait()
        take = pl.ds(i * block, block)
        high, low = split(held_ref[take, columns])
        high_ref[take] = high
        low_ref[take] = low
        value = project_block(high, low, both_ref[take])
        store(out_ref, value, add=i > 0)


def project_first(image, row_factor, width, packed, blocks=2):
    rows, rank = row_factor.shape
    return pl.pallas_call(
        first_kernel,
        in_specs=[pl.BlockSpec(memory_space=pl.ANY), pl.BlockSpec(memory_space=pl.ANY)],
        out_shape=(
            jax.ShapeDtypeStruct(packed, F32),
            jax.ShapeDtypeStruct((rows, width), BF16),
            jax.ShapeDtypeStruct((rows, width), BF16),
            jax.ShapeDtypeStruct(image.shape, F32),
            jax.ShapeDtypeStruct((rows, 2 * rank), BF16),
        ),
        scratch_shapes=[
            pltpu.VMEM((rows, rank), F32),
            pltpu.SemaphoreType.DMA((blocks,)),
            pltpu.SemaphoreType.DMA,
        ],
        compiler_params=SMALL,
        name="project_first",
    )(
        pltpu.with_memory_space_constraint(image, pltpu.HBM),
        pltpu.with_memory_space_constraint(row_factor, pltpu.HBM),
    )


def second_kernel(blocks, held_ref, both_ref, out_ref, high_ref, low_ref):
    rows, width = high_ref.shape
    block = rows // blocks
    columns = columns_of(0, width)
    total = None
    for i in range(blocks):
        take = pl.ds(i * block, block)
        high, low = split(held_ref[take, columns])
        high_ref[take] = high
        low_ref[take] = low
        value = project_block(high, low, both_ref[take])
        total = value if total is None else total + value
    store(out_ref, total)


def project_second(held, both, width, packed, blocks=4):
    rows, rank = both.shape[0], both.shape[1] // 2
    return pl.pallas_call(
        functools.partial(second_kernel, blocks),
        out_shape=(
            jax.ShapeDtypeStruct(packed, F32),
            jax.ShapeDtypeStruct((rows, width), BF16),
            jax.ShapeDtypeStruct((rows, width), BF16),
        ),
        cost_estimate=pl.CostEstimate(
            flops=6 * rows * width * rank, bytes_accessed=4 * rows * (width + rank), transcendentals=0
        ),
        compiler_params=SMALL,
        name="project_second",
    )(held, both)


def product_kernel(blocks, high_ref, low_ref, weight_ref, *refs):
    out_ref = refs[-1]
    weight_high, weight_low = split(load(weight_ref))
    rank = weight_high.shape[0]
    both = jnp.concatenate([weight_high, weight_low], axis=0)
    block = out_ref.shape[0] // blocks
    for i in range(blocks):
        take = pl.ds(i * block, block)
        wide = fastdot(high_ref[take], both, ((1,), (1,)))
        value = wide[:, :rank] + wide[:, rank:] + fastdot(low_ref[take], weight_high, ((1,), (1,)))
        if len(refs) > 1:
            value = value + refs[0][take]
        out_ref[take] = value


def multiply(high, low, weight, start=None, blocks=4):
    rows, width = high.shape
    rank = weight.size // width
    more = () if start is None else (start,)
    return pl.pallas_call(
        functools.partial(product_kernel, blocks),
        out_shape=jax.ShapeDtypeStruct((rows, rank), F32),
        cost_estimate=pl.CostEstimate(
            flops=6 * rows * width * rank, bytes_accessed=4 * rows * (width + rank), transcendentals=0
        ),
        compiler_params=SMALL,
        name="multiply",
    )(high, low, weight, *more)


def cells(rows, count, row_of, cell_of):
    row = row_of(lax.broadcasted_iota(jnp.int32, (rows, count), 0))
    return (row == cell_of(lax.broadcasted_iota(jnp.int32, (rows, count), 1))).astype(F32)


def spread(groups_n, rank):
    per = rank // groups_n
    return cells(rank, groups_n, lambda row: row // per, lambda cell: cell)


def same_slot(groups_n, rank):
    per = rank // groups_n
    return cells(rank, rank, lambda row: row % per, lambda cell: cell % per) > 0.5


def gram_kernel(groups_n, owned_ref, out_ref):
    high, low = split(load(owned_ref))
    rank = high.shape[0]
    per = rank // groups_n
    wide = fastdot(high, jnp.concatenate([high, low], axis=0), ((1,), (1,)))
    full = wide[:, :rank] + wide[:, rank:] + wide[:, rank:].T
    full = jnp.where(same_slot(groups_n, rank), full, 0.0)
    if len(out_ref.shape) == 2:
        fold = spread(groups_n, rank)
        out_ref[...] = dot(dot(fold, full, ((0,), (0,))), fold)
    else:
        count = out_ref.shape[2]
        columns = cells(rank, count, lambda row: row // per, lambda cell: cell % groups_n).astype(BF16)
        folded = fastdot(
            jnp.concatenate(split3(full), axis=1), jnp.concatenate([columns, columns, columns], axis=0), ((1,), (0,))
        )
        rows = cells(rank, count, lambda row: row // per, lambda cell: cell // groups_n)
        flat = jnp.sum(rows * folded, axis=0, keepdims=True)
        out_ref[...] = jnp.broadcast_to(flat[None], out_ref.shape)


def small_gram(owned, groups_n, shape):
    return pl.pallas_call(
        functools.partial(gram_kernel, groups_n),
        out_shape=jax.ShapeDtypeStruct(shape, F32),
        compiler_params=SMALL,
        name="small_gram",
    )(owned)


def mix_kernel(groups_n, gram_ref, time_ref, owned_ref, out_ref, time_out_ref):
    owned_high, owned_low = split(load(owned_ref))
    rank = owned_high.shape[0]
    per = rank // groups_n
    if len(gram_ref.shape) == 2:
        fold = spread(groups_n, rank)
        start = dot(fold, dot(gram_ref[...], time_ref[...], ((1,), (1,))))
        turned = dot(dot(time_ref[...], gram_ref[...], ((1,), (1,))), fold, ((1,), (1,)))
    else:
        count = gram_ref.shape[2]
        flat = jnp.sum(gram_ref[...], axis=0)
        rows = cells(rank, count, lambda row: row // per, lambda cell: cell // groups_n) * flat
        columns = dot(time_ref[...], cells(groups_n, count, lambda row: row, lambda cell: cell % groups_n))
        start = dot(rows, columns, ((1,), (1,)))
        turned = dot(columns, rows, ((1,), (1,)))
    factor = orth_factor(dot(turned, start) * (1.0 / per))
    size = factor.shape[0]
    if size <= 16:
        basis = tree_sum([start[:, k : k + 1] * factor[k : k + 1] for k in range(size)])
        basis_turned = tree_sum([factor[:, k : k + 1] * turned[k : k + 1] for k in range(size)])
        outer = tree_sum([basis[:, k : k + 1] * basis_turned[k : k + 1] for k in range(size)])
    else:
        basis = dot(start, factor)
        outer = dot(basis, basis, ((1,), (1,)))
    mixer = jnp.where(same_slot(groups_n, rank), outer, 0.0)
    mixer_high, mixer_low = split(mixer)
    mixed = fastdot(
        jnp.concatenate([mixer_high, mixer_low, mixer_high], axis=1),
        jnp.concatenate([owned_high, owned_high, owned_low], axis=0),
        ((1,), (0,)),
    )
    store(out_ref, mixed)
    one_of_each = cells(groups_n, rank, lambda row: row * per, lambda cell: cell)
    time_out_ref[...] = dot(one_of_each, basis) * math.sqrt(groups_n)


def mix(gram, time_factor, owned, groups_n):
    return pl.pallas_call(
        functools.partial(mix_kernel, groups_n),
        out_shape=(jax.ShapeDtypeStruct(owned.shape, F32), jax.ShapeDtypeStruct(time_factor.shape, F32)),
        compiler_params=SMALL,
        name="mix",
    )(gram, time_factor.T, owned)


def finish_kernel(scale, blocks, block_ref, mine_ref, other_ref, out_ref, made_ref, sems):
    rows = block_ref.shape[0] // blocks
    high, middle, low = split3(block_ref[...])
    left, left_more = jnp.concatenate([high, middle], axis=1), jnp.concatenate([high, low], axis=1)
    high, middle, low = split3(orth_factor(mine_ref[...] + other_ref[...]) * scale)
    both = jnp.concatenate([high, middle], axis=1)
    right, right_more = jnp.concatenate([both, both], axis=0), jnp.concatenate([low, high], axis=0)
    copies = []
    for i in range(blocks):
        take = pl.ds(i * rows, rows)
        part = slice(i * rows, (i + 1) * rows)
        made_ref[take] = by_stacked(left[part], right) + fastdot(left_more[part], right_more, ((1,), (0,)))
        copies.append(pltpu.make_async_copy(made_ref.at[take], out_ref.at[take], sems.at[i]))
        copies[-1].start()
    for copy in copies:
        copy.wait()


def finish(block, mine, other, scale, blocks=4):
    return pl.pallas_call(
        functools.partial(finish_kernel, scale, blocks),
        out_shape=jax.ShapeDtypeStruct(block.shape, F32),
        out_specs=pl.BlockSpec(memory_space=pl.ANY),
        scratch_shapes=[pltpu.VMEM(block.shape, F32), pltpu.SemaphoreType.DMA((blocks,))],
        compiler_params=SMALL,
        name="finish",
    )(block, mine, other)


def row_gram_kernel(block_ref, out_ref):
    high, low = split(block_ref[...])
    rank = high.shape[1]
    wide = fastdot(high, jnp.concatenate([high, low], axis=1), ((0,), (0,)))
    out_ref[...] = wide[:, :rank] + wide[:, rank:] + wide[:, rank:].T


def row_gram(block):
    rank = block.shape[1]
    return pl.pallas_call(row_gram_kernel, out_shape=jax.ShapeDtypeStruct((rank, rank), F32), compiler_params=SMALL, name="row_gram")(block)


def make_on_device(groups_n, reps):
    half_n = groups_n // 2
    halves = [[h * half_n + i for i in range(half_n)] for h in range(2)]
    across = [(i, (i + half_n) % groups_n) for i in range(groups_n)]
    swap = [(0, 1), (1, 0)]

    def all_to_all(value, parts, groups=None):
        shape = value.shape
        value = value.reshape((parts, shape[0] // parts) + shape[1:])
        value = lax.all_to_all(value, "grp", split_axis=0, concat_axis=0, tiled=True, axis_index_groups=groups)
        return value.reshape(shape)

    def to_owners(value):
        if len(value.shape) == 2:
            return all_to_all(value, groups_n)
        flat = value.reshape((groups_n * reps,) + value.shape[2:])
        return lax.all_to_all(flat, ("grp", "rep"), split_axis=0, concat_axis=0, tiled=True).reshape(value.shape)

    def on_device(snapshots, row_factor, time_factor):
        rows, cols = snapshots.shape[1:]
        rank = row_factor.shape[1]
        width = cols // reps
        fits = rank % (8 * groups_n) == 0 and width % (128 * reps) == 0
        packed = packed_shape(groups_n, reps if fits else 1, rank, width)
        send, far_high, far_low, held, both = project_first(snapshots[0], row_factor, width, packed)
        received = lax.ppermute(send, "rep", swap)
        summed, near_high, near_low = project_second(held, both, width, packed)
        summed = summed + received
        owned = to_owners(summed)
        devices = groups_n * reps
        if devices * groups_n * groups_n <= 1 << 20:
            grams = lax.all_to_all(
                small_gram(owned, groups_n, (devices, 1, groups_n * groups_n)),
                ("grp", "rep"),
                split_axis=0,
                concat_axis=0,
                tiled=True,
            )
        else:
            grams = lax.psum(small_gram(owned, groups_n, (groups_n, groups_n)), ("grp", "rep"))
        weights, new_time = mix(grams, time_factor, owned, groups_n)
        weight = to_owners(weights)
        other_weight = lax.ppermute(weight, "rep", swap)
        product = multiply(far_high, far_low, other_weight, multiply(near_high, near_low, weight))
        parts = all_to_all(product, half_n, halves)
        chunk = jnp.sum(parts.reshape(half_n, rows // half_n, rank), axis=0)
        chunk = chunk + lax.ppermute(chunk, "grp", across)
        block = all_to_all(jnp.tile(chunk, (half_n, 1)), half_n, halves)
        gram = row_gram(block)
        new_rows = finish(block, gram, lax.ppermute(gram, "rep", swap), math.sqrt(rows * reps))
        return (new_rows, new_time)

    return on_device


def solution(mesh):
    return jax.shard_map(
        make_on_device(mesh.shape["grp"], mesh.shape["rep"]),
        mesh=mesh,
        in_specs=(P("grp", "rep", None), P("rep", None), P()),
        out_specs=(P("rep", None), P()),
        check_vma=False,
    )
```
